32 devices in a mesh: seq: 8 (over z, x), tp: 4 (over y, core).
Axes of the slice: x: 2, y: 2, z: 4, core: 2. Of those that a mesh axis runs over, the one named last changes fastest.
Arguments:
- packed_input: int32 [512, 5120], P('seq', 'tp'), may hold values from -2147483648 to 2147483646
- block_exponent: int32 [40, 4096], P('tp', 'seq'), may hold values from -5 to -1
- gate_input: bfloat16 [4096, 5120], P('seq', 'tp'), may hold values from -80 to 80
- state_write: bfloat16 [4096, 128], P('seq'), may hold values from -6 to 6
- state_read: bfloat16 [4096, 128], P('seq'), may hold values from -6 to 6
- log_decay: float32 [80, 4096], P('tp', 'seq'), may hold values from -1.6 to 0
- skip_weight: float32 [80], P('tp'), may hold values from 0.3 to 3
- norm_gain: float32 [5120], P('tp'), may hold values from 0.5 to 1.5
- out_weight: bfloat16 [5120, 2560], P('tp'), may hold values from -0.078125 to 0.078125
- out_cotangent: bfloat16 [4096, 2560], P('seq', 'tp'), may hold values from -6 to 6
Outputs:
- grad_input: bfloat16 [4096, 5120], P('seq', 'tp')
- grad_gate: bfloat16 [4096, 5120], P('seq', 'tp')
- grad_write: float32 [4096, 128], P('seq')
- grad_read: float32 [4096, 128], P('seq')
- grad_decay: float32 [80, 4096], P('tp', 'seq')
- grad_skip: float32 [80], P('tp')
- grad_gain: float32 [5120], P('tp')
- grad_out_weight: float32 [5120, 2560], P('tp', 'seq')
The draws below stay inside these ranges and needn't reach their ends.
All inputs are finite; a program needn't handle non-finite values.
Results may differ from the reference program's by a relative error of at most 0.0049.
Values may be sent and summed in bfloat16 or wider, within the bound.
A program may use at most 128 MiB of HBM per device.

```python
import math
import jax
import jax.numpy as jnp
from jax import lax

D = 2560
HEAD_NUMBER = 80
N = 128
QBLOCK = 128
TOK_DEV = 512
TOKEN_NUMBER = 4096
HP = 5120


def draw_gate_input(key, part):
    first_key, second_key = jax.random.split(jax.random.fold_in(key, 11))
    column_pos = jnp.arange(HP, dtype=jnp.float32) / (HP - 1)
    base = jax.random.truncated_normal(first_key, -4.0, 4.0, (TOKEN_NUMBER, HP), jnp.float32)
    column_scale = 3.0 ** column_pos
    row_scale = jnp.exp(jax.random.uniform(second_key, (TOKEN_NUMBER, 1), jnp.float32, math.log(0.3), math.log(3.0)))
    return (base * column_scale[None, :] * row_scale).astype(jnp.bfloat16)


def draw_log_decay(key, part):
    random_keys = jax.random.split(jax.random.fold_in(key, 23), 7)
    slow_share = 0.5
    is_slow = jax.random.uniform(random_keys[0], (HEAD_NUMBER, 1), jnp.float32) < slow_share
    slow_rate = jax.random.uniform(random_keys[1], (HEAD_NUMBER, 1), jnp.float32, 0.15, 0.6) / TOKEN_NUMBER
    fast_rate = jnp.exp(jax.random.uniform(random_keys[2], (HEAD_NUMBER, 1), jnp.float32, math.log(1.0 / 50.0), math.log(1.0 / 30.0)))
    baseline_rate = jnp.where(is_slow, slow_rate, fast_rate)
    coarse_values = jnp.exp(jax.random.uniform(random_keys[3], (HEAD_NUMBER, TOKEN_NUMBER), jnp.float32, math.log(0.5), math.log(2.0)))
    block_multiplier = jnp.exp(jax.random.uniform(random_keys[4], (HEAD_NUMBER, TOKEN_NUMBER // TOK_DEV), jnp.float32, math.log(0.5), math.log(2.0)))
    block_multiplier = jnp.repeat(block_multiplier, TOK_DEV, axis=1)
    spike_position = jax.random.randint(random_keys[5], (HEAD_NUMBER, 2), 0, TOKEN_NUMBER)
    spike_magnitude = jax.random.uniform(random_keys[6], (HEAD_NUMBER, 2), jnp.float32, 0.22, 0.69)
    token_places = jnp.arange(TOKEN_NUMBER)[None, :]
    spike_list = jnp.where(token_places == spike_position[:, 0:1], spike_magnitude[:, 0:1], 0.0) + jnp.where(token_places == spike_position[:, 1:2], spike_magnitude[:, 1:2], 0.0)
    return -(baseline_rate * coarse_values * block_multiplier + spike_list)


def set_ends(entries, rng, least, high):
    longest = entries.shape.index(max(entries.shape))
    spots = []
    for shift in (0, 1):
        where = [jax.random.randint(jax.random.fold_in(rng, axis), (), 0, length) for axis, length in enumerate(entries.shape)]
        where[longest] = (where[longest] + shift) % entries.shape[longest]
        spots.append(tuple(where))
    return entries.at[spots[0]].set(least).at[spots[1]].set(high)


def levels(rng, shape, cuts, low, high):
    gain = 1.0
    for axis_at, parts in cuts:
        steps = jax.random.uniform(jax.random.fold_in(jax.random.fold_in(rng, 6), axis_at), (parts,), jnp.float32, low / len(cuts), high / len(cuts))
        gain = gain * jnp.repeat(jnp.exp(steps), shape[axis_at] // parts).reshape((-1,) + (1,) * (len(shape) - 1 - axis_at))
    return gain


def bell_draw(stream_key, extent, scale, limit, pieces=(), kind=jnp.bfloat16):
    drawn = jax.random.normal(stream_key, extent, jnp.float32) * scale
    if len(pieces) > 0:
        drawn = levels(stream_key, extent, pieces, -0.22, 0.18) * drawn
    return jnp.clip(drawn, min=-limit, max=limit).astype(kind)


def setup_inputs(seed: int = 0) -> dict:
    splits = jax.random.split(jax.random.key(seed), 11)
    return {
        "packed_input": set_ends(jax.random.randint(splits[0], (TOKEN_NUMBER // 8, HP), -2147483648, 2147483647), jax.random.fold_in(splits[0], 1), -2147483648, 2147483646).astype(jnp.int32),
        "block_exponent": set_ends(jax.random.randint(splits[1], (HP // QBLOCK, TOKEN_NUMBER), -5, 0), jax.random.fold_in(splits[1], 1), -5, -1).astype(jnp.int32),
        "gate_input": draw_gate_input(jax.random.fold_in(splits[10], 71), 0),
        "state_write": bell_draw(splits[3], (TOKEN_NUMBER, N), 1.0, 6.0, ((0, 8),)),
        "state_read": bell_draw(splits[4], (TOKEN_NUMBER, N), 1.0, 6.0, ((0, 8),)),
        "log_decay": draw_log_decay(jax.random.fold_in(splits[10], 71), 0),
        "skip_weight": jnp.clip(jnp.exp(math.log(3.0) - 2.3025851 * jax.random.uniform(splits[6], (HEAD_NUMBER,), jnp.float32) ** levels(splits[6], (HEAD_NUMBER,), ((0, 4),), -0.2, 0.2)), 0.3, 3.0),
        "norm_gain": jnp.clip(1.0 + 0.1 * jax.random.normal(splits[7], (HP,), jnp.float32), 0.5, 1.5),
        "out_weight": bell_draw(splits[8], (HP, D), HP ** -0.5, 0.078125, ((0, 4),)),
        "out_cotangent": bell_draw(splits[9], (TOKEN_NUMBER, D), 1.0, 6.0, ((0, 8), (1, 4))),
    }


PRECISE = lax.Precision.HIGHEST

def dequantize(packed_words, exponents):
    shifts = 4 * jnp.arange(8, dtype=jnp.int32)
    fields = jnp.bitwise_and(jnp.right_shift(packed_words[:, None, :], shifts[None, :, None]), 15) - 8
    fields = fields.reshape(packed_words.shape[0] * 8, packed_words.shape[1])
    factors = jnp.exp2(exponents.astype(jnp.float32))
    group_width = fields.shape[1] // exponents.shape[0]
    factors = jnp.repeat(factors.T, group_width, axis=1)
    return (fields.astype(jnp.float32) * factors).astype(jnp.bfloat16)

def lower_decays(seg_sum):
    length = seg_sum.shape[1]
    is_lower = (jnp.arange(length)[:, None] >= jnp.arange(length)[None, :])[None]
    spread = seg_sum[:, :, None] - seg_sum[:, None, :]
    return jnp.where(is_lower, jnp.exp(jnp.where(is_lower, spread, 0.0)), 0.0)

def block_step(state_now, inputs):
    x_part, decay_part, write_part, read_part = inputs
    seg_sum = jnp.cumsum(decay_part, axis=1)
    mixing = lower_decays(seg_sum) * jnp.dot(read_part, write_part.T, precision=PRECISE)[None]
    carried_in = jnp.einsum('in,hpn->ihp', read_part, state_now, precision=PRECISE)
    result = jnp.einsum('hij,jhp->ihp', mixing, x_part, precision=PRECISE) + jnp.exp(seg_sum).T[:, :, None] * carried_in
    end_weight = jnp.exp(seg_sum[:, -1:] - seg_sum)
    state_next = jnp.exp(seg_sum[:, -1])[:, None, None] * state_now + jnp.einsum('jhp,jn->hpn', x_part * end_weight.T[:, :, None], write_part, precision=PRECISE)
    return (state_next, result)

def scan_states(x_heads, log_decay, write_rows, read_rows):
    total, head_count, head_width = x_heads.shape
    block_len = min(256, TOK_DEV)
    blocks = total // block_len
    x_blocks = x_heads.reshape(blocks, block_len, head_count, head_width)
    decay_blocks = log_decay.reshape(head_count, blocks, block_len).transpose(1, 0, 2)
    write_blocks = write_rows.reshape(blocks, block_len, -1)
    read_blocks = read_rows.reshape(blocks, block_len, -1)
    initial = jnp.zeros((head_count, head_width, write_rows.shape[1]), jnp.float32)
    _, outputs = lax.scan(jax.checkpoint(block_step), initial, (x_blocks, decay_blocks, write_blocks, read_blocks))
    return outputs.reshape(total, head_count, head_width)

def add_block(running, pair):
    part_sum = jnp.dot(pair[0].T, pair[1], preferred_element_type=jnp.float32)
    rounded = lax.optimization_barrier(part_sum.astype(jnp.bfloat16))
    return (running + rounded.astype(jnp.float32), None)

def reference(packed_input, block_exponent, gate_input, state_write, state_read, log_decay, skip_weight, norm_gain, out_weight, out_cotangent):
    x_values = dequantize(packed_input, block_exponent)
    total, width = x_values.shape
    head_count = log_decay.shape[0]
    x_heads = x_values.astype(jnp.float32).reshape(total, head_count, width // head_count)
    write_rows = state_write.astype(jnp.float32)
    read_rows = state_read.astype(jnp.float32)
    core, pullback = jax.vjp(scan_states, x_heads, log_decay, write_rows, read_rows)
    y_full = (core + skip_weight[None, :, None] * x_heads).reshape(total, width)
    gate = gate_input.astype(jnp.float32)
    sigma = jax.nn.sigmoid(gate)
    active = gate * sigma
    mixed = y_full * active
    scale_row = lax.rsqrt(lax.optimization_barrier(jnp.mean(mixed * mixed, axis=1, keepdims=True)) + 1e-05)
    normed = (mixed * scale_row * norm_gain).astype(jnp.bfloat16)
    grad_v = jnp.dot(out_cotangent, out_weight.T, preferred_element_type=jnp.float32)
    model_width = out_weight.shape[1]
    normed_blocks = normed.reshape(-1, TOK_DEV, width)
    cot_blocks = out_cotangent.reshape(-1, TOK_DEV, model_width)
    grad_out_weight, _ = lax.scan(add_block, jnp.zeros((width, model_width), jnp.float32), (normed_blocks, cot_blocks))
    scaled = grad_v * norm_gain
    grad_gain = lax.optimization_barrier(jnp.sum(grad_v * mixed * scale_row, axis=0))
    inner = lax.optimization_barrier(jnp.sum(scaled * mixed, axis=1, keepdims=True))
    grad_mixed = scale_row * scaled - mixed * (scale_row * scale_row * scale_row) * inner / width
    grad_gate = (grad_mixed * y_full * sigma * (1.0 + gate * (1.0 - sigma))).astype(jnp.bfloat16)
    grad_y = (grad_mixed * active).reshape(total, head_count, width // head_count)
    grad_skip = lax.optimization_barrier(jnp.sum(grad_y * x_heads, axis=(0, 2)))
    grad_core, grad_decay, grad_write, grad_read = pullback(grad_y)
    grad_input = (grad_core + skip_weight[None, :, None] * grad_y).reshape(total, width).astype(jnp.bfloat16)
    return (grad_input, grad_gate, grad_write, grad_read, grad_decay, grad_skip, grad_gain, grad_out_weight)
```

```python
import functools

import jax
import jax.numpy as jnp
from jax import lax
from jax.experimental import pallas as pl
from jax.experimental.pallas import tpu as pltpu
from jax.sharding import PartitionSpec as P

PRECISE = lax.Precision.HIGHEST
F32 = jnp.float32
BF16 = jnp.bfloat16
LANES = 128
CHUNK = 128
VMEM_LIMIT = 48 * 1024 * 1024
TAIL_VMEM = 62 * 1024 * 1024
MESH = pl.DeviceIdType.MESH

FACTOR, SEG, SEG_EXP, TO_CHUNK_END, FROM_START, TO_END = 0, 1, 3, 5, 7, 9
COLUMN_COUNT = 16


def dot(a, b, contract):
    return lax.dot_general(a, b, ((contract[:1], contract[1:]), ((), ())), preferred_element_type=F32)


def spread_pair(columns, at, rows):
    lane = lax.broadcasted_iota(jnp.int32, (rows, LANES), 1)
    return jnp.where(lane < LANES // 2, columns[:, at : at + 1], columns[:, at + 1 : at + 2])


def chunk_decay(columns, seg_rows, head, rows):
    token = lax.broadcasted_iota(jnp.int32, (rows, rows), 0)
    source = lax.broadcasted_iota(jnp.int32, (rows, rows), 1)
    spread = columns[:, SEG + head : SEG + head + 1] - seg_rows[SEG + head : SEG + head + 1, :]
    return jnp.exp(jnp.where(token >= source, spread, -1e30))


def unpack_kernel(packed_ref, col_ref, write_t_ref, x_ref, state_ref):
    words = packed_ref[...]
    groups = words.shape[0]
    length = groups * 8
    wide = jnp.broadcast_to(words[:, None, :], (groups, 8, LANES))
    shifts = 4 * lax.broadcasted_iota(jnp.int32, (groups, 8, LANES), 1)
    fields = jnp.bitwise_and(jnp.right_shift(wide, shifts), 15) - 8
    columns = col_ref[0]
    x = fields.astype(F32).reshape(length, LANES) * columns[:, FACTOR : FACTOR + 1]
    x_ref[...] = x.astype(BF16)
    weighted = (x * spread_pair(columns, TO_END, length)).astype(BF16)
    state_ref[...] = dot(write_t_ref[...], weighted, (1, 0)).astype(BF16)


def local_kernel(x_ref, col_ref, seg_ref, row_ref, cross_ref, write_t_ref, read_ref, y_ref):
    length = x_ref.shape[0]
    chunk = min(CHUNK, length)
    lane = lax.broadcasted_iota(jnp.int32, (chunk, LANES), 1)
    state = None
    for c in range(length // chunk):
        part = pl.ds(c * chunk, chunk)
        columns = col_ref[0, part, :]
        seg_rows = seg_ref[0, :, part]
        x = x_ref[part, :]
        cross = cross_ref[c]
        halves = []
        for head in range(2):
            mixing = (chunk_decay(columns, seg_rows, head, chunk) * cross).astype(BF16)
            halves.append(dot(mixing, x, (1, 0)))
        y = jnp.where(lane < LANES // 2, halves[0], halves[1])
        if state is not None:
            y = y + spread_pair(columns, SEG_EXP, chunk) * dot(
                read_ref[part, :], state.astype(BF16), (1, 0)
            )
        y_ref[part, :] = y
        weighted = (x.astype(F32) * spread_pair(columns, TO_CHUNK_END, chunk)).astype(BF16)
        added = dot(write_t_ref[:, part], weighted, (1, 0))
        state = added if state is None else state * row_ref[0, c + 3 : c + 4, :] + added


def weigh_pieces(piece_ref, weight_ref):
    total = None
    for k in range(piece_ref.shape[0]):
        term = piece_ref[k].astype(F32) * weight_ref[0, k : k + 1, :]
        total = term if total is None else total + term
    return total


def mix_kernel(
    y_local_ref, x_ref, col_ref, row_ref, read_ref, piece_ref, weight_ref, gate_ref, grad_v_ref,
    y_ref, state_ref, square_ref, inner_ref,
):
    length = x_ref.shape[0]
    state = weigh_pieces(piece_ref, weight_ref)
    state_ref[...] = state
    carried = dot(read_ref[...], state.astype(BF16), (1, 0))
    y = (
        y_local_ref[...]
        + spread_pair(col_ref[0], FROM_START, length) * carried
        + row_ref[0, 0:1, :] * x_ref[...].astype(F32)
    )
    y_ref[...] = y
    gate = gate_ref[...].astype(F32)
    mixed = y * gate * jax.nn.sigmoid(gate)
    square = mixed * mixed
    inner = grad_v_ref[...] * row_ref[0, 1:2, :] * mixed

    @pl.when(pl.program_id(0) == 0)
    def _():
        square_ref[...] = square
        inner_ref[...] = inner

    @pl.when(pl.program_id(0) > 0)
    def _():
        square_ref[...] += square
        inner_ref[...] += inner


def gate_kernel(
    y_ref, x_ref, col_ref, row_ref, read_t_ref, gate_ref, grad_v_ref, scale_ref,
    normed_ref, grad_gate_ref, grad_y_ref, sums_ref, cot_ref,
):
    length = x_ref.shape[0]
    scale = scale_ref[:, 0:1]
    pull = scale_ref[:, 1:2]
    gain = row_ref[0, 1:2, :]
    y = y_ref[...]
    gate = gate_ref[...].astype(F32)
    sigma = jax.nn.sigmoid(gate)
    active = gate * sigma
    mixed = y * active
    mixed_scaled = mixed * scale
    normed_ref[...] = (mixed_scaled * gain).astype(BF16)
    grad_v = grad_v_ref[...]
    grad_mixed = scale * grad_v * gain - mixed * pull
    grad_gate_ref[...] = (grad_mixed * y * sigma * (1.0 + gate * (1.0 - sigma))).astype(BF16)
    grad_y = grad_mixed * active
    grad_y_ref[...] = grad_y.astype(BF16)
    gain_sum = jnp.sum(grad_v * mixed_scaled, axis=0, keepdims=True)
    skip_sum = jnp.sum(grad_y * x_ref[...].astype(F32), axis=0, keepdims=True)
    sums_ref[0, 0:1, :] = gain_sum
    sums_ref[0, 1:2, :] = skip_sum
    weighted = (grad_y * spread_pair(col_ref[0], FROM_START, length)).astype(BF16)
    cot_ref[...] = dot(read_t_ref[...], weighted, (1, 0)).astype(BF16)


def chip_rows(sequence):
    return max(d for d in range(1, sequence + 1) if d * d <= sequence and sequence % d == 0)


def visit(z, depth, step):
    low = jnp.minimum(z, depth - 1 - z)
    late = jnp.maximum(step - (depth - 1 - 2 * low), 0)
    half = lax.div(late, 2)
    near = jnp.where(lax.rem(late, 2) == 0, 2 * low - half, half)
    target = jnp.where(step < depth - 1 - 2 * low, depth - 1 - step, near)
    return jnp.where(2 * z <= depth - 1, target, depth - 1 - target)


def lanes_of(pair):
    return pl.ds(pl.multiple_of(pair * LANES, LANES), LANES)


def greet(axes):
    barrier = pltpu.get_barrier_semaphore()
    count = 0
    for axis, size in axes:
        me = lax.axis_index(axis)
        for step in range(1, size):
            pl.semaphore_signal(
                barrier, inc=1, device_id={axis: lax.rem(me + step, size)}, device_id_type=MESH
            )
            count += 1
    pl.semaphore_wait(barrier, count)


def remote(source, target, sems, axis, peer):
    return pltpu.make_async_remote_copy(
        src_ref=source, dst_ref=target, send_sem=sems[0], recv_sem=sems[1],
        device_id={axis: peer}, device_id_type=MESH,
    )


def tail_kernel(
    sequence, tensor,
    normed_ref, cot_ref, local_ref, decay_ref, sums_ref, seg_ref, row_ref, cross_ref, write_ref,
    read_ref, write_t_ref, read_t_ref, state_ref, x_hbm, grad_y_hbm, y_hbm, col_hbm,
    grad_x_ref, grad_map_ref, diff_ref, const_ref, weight_ref, total_ref,
    own, part, arrived, up_out, up_in, down_out, down_in, acc, piece, piece_decay, chain_in,
    chain_out, carry_ref, gathered, map_acc, map_in, summed_ref, x_ref, grad_y_ref, y_ref, col_ref,
    part_sems, up_sems, down_sems, piece_sems, decay_sems, chain_sems, sum_sems, map_sems, share_sems,
    local_sems,
):
    row = chip_rows(sequence)
    depth = sequence // row
    me = lax.axis_index("seq")
    mine = lax.axis_index("tp")
    z, place = lax.div(me, row), lax.rem(me, row)
    length, width = normed_ref.shape
    pairs = width // LANES
    columns_out = weight_ref.shape[1]
    chunk = min(CHUNK, length)
    chunks = length // chunk

    fetches = [
        pltpu.make_async_copy(source, target, local_sems.at[i])
        for i, (source, target) in enumerate(
            [(x_hbm, x_ref), (grad_y_hbm, grad_y_ref), (y_hbm, y_ref), (col_hbm, col_ref)]
        )
    ]
    for fetch in fetches:
        fetch.start()
    greet((("seq", sequence), ("tp", tensor)))

    def neighbour(step):
        return z * row + lax.rem(place + step, row)

    exchanges = []
    for step in range(1, row):
        exchanges.append(
            remote(
                local_ref, piece.at[place],
                (piece_sems.at[0, step - 1], piece_sems.at[1, step - 1]), "seq", neighbour(step),
            )
        )
        exchanges.append(
            remote(
                decay_ref, piece_decay.at[place],
                (decay_sems.at[0, step - 1], decay_sems.at[1, step - 1]), "seq", neighbour(step),
            )
        )
    sum_copies = [
        remote(
            sums_ref, gathered.at[me], (sum_sems.at[0, step - 1], sum_sems.at[1, step - 1]), "seq",
            lax.rem(me + step, sequence),
        )
        for step in range(1, sequence)
    ]
    for copy in exchanges + sum_copies:
        copy.start()
    piece[place] = local_ref[...]
    piece_decay[place] = decay_ref[...]
    gathered[me] = sums_ref[...]

    def part_copy(target_z, step):
        return remote(
            part.at[target_z, step - 1], arrived.at[target_z, step - 1],
            (part_sems.at[0, target_z, step - 1], part_sems.at[1, target_z, step - 1]), "seq",
            neighbour(step),
        )

    def multiply(step, _):
        target_z = visit(z, depth, step)
        for offset in list(range(1, row)) + [0]:
            block = target_z * row + lax.rem(place + offset, row)
            taken = cot_ref[pl.ds(pl.multiple_of(block * columns_out, 16), columns_out), :]
            for at in range(0, width, 2 * LANES):
                span = pl.ds(at, min(2 * LANES, width - at))
                product = dot(taken, normed_ref[:, span], (1, 0)).astype(BF16)
                if offset:
                    part[target_z, offset - 1, :, span] = product
                else:
                    own[target_z, :, span] = product
            if offset:
                part_copy(target_z, offset).start()
        return 0

    lax.fori_loop(0, depth, multiply, 0)

    for copy in exchanges:
        copy.wait_recv()
    bounds = [0, (pairs + 1) // 2, pairs]
    for half in range(2):
        first, last = bounds[half], bounds[half + 1]
        span = pl.ds(first * LANES, (last - first) * LANES)
        hop = remote(
            chain_out.at[:, span], chain_in.at[:, span],
            (chain_sems.at[0, half], chain_sems.at[1, half]), "seq", me - row,
        )

        def link(entering):
            def one(pair, _):
                lanes = lanes_of(pair)
                group, after = None, jnp.zeros((piece.shape[1], LANES), F32)
                scale, factor = None, jnp.ones((1, LANES), F32)
                for at in reversed(range(row)):
                    term = piece[at, :, lanes].astype(F32)
                    decay = piece_decay[at, :, lanes]
                    take = at > place
                    after = jnp.where(take, term + decay * after, after)
                    factor = jnp.where(take, decay * factor, factor)
                    group = term if group is None else term + decay * group
                    scale = decay if scale is None else decay * scale
                if entering:
                    incoming = chain_in[:, lanes].astype(F32)
                    group = group + scale * incoming
                    after = after + factor * incoming
                carry_ref[:, lanes] = after
                chain_out[:, lanes] = group.astype(BF16)
                return 0

            lax.fori_loop(first, last, one, 0)

        @pl.when(z == depth - 1)
        def _():
            link(False)

        @pl.when(z < depth - 1)
        def _():
            hop.wait_recv()
            link(True)

        @pl.when(z > 0)
        def _():
            hop.start()

    def relay(step, up):
        target_z = z + (depth - 1 - step) if up else z - (depth - 1) + step
        outgoing, incoming, sems = (up_out, up_in, up_sems) if up else (down_out, down_in, down_sems)
        is_end = z == 0 if up else z == depth - 1
        is_active = z <= step if up else z >= depth - 1 - step

        def copy(at):
            return remote(
                outgoing.at[at], incoming.at[at], (sems.at[0, at], sems.at[1, at]), "seq",
                me + row if up else me - row,
            )

        def add(more):
            def one(pair, _):
                lanes = lanes_of(pair)
                value = own[target_z, :, lanes].astype(F32)
                for at in range(row - 1):
                    value = value + arrived[target_z, at, :, lanes].astype(F32)
                if more:
                    value = value + incoming[step - 1, :, lanes].astype(F32)
                outgoing[step, :, lanes] = value.astype(BF16)
                return 0

            lax.fori_loop(0, pairs, one, 0)

        @pl.when(is_end)
        def _():
            add(False)

        if step > 0:

            @pl.when(jnp.logical_and(is_active, jnp.logical_not(is_end)))
            def _():
                copy(step - 1).wait_recv()
                add(True)

        @pl.when(is_active)
        def _():
            copy(step).start()

        return copy, is_active

    def serve(step):
        target_z = visit(z, depth, step)
        for offset in range(1, row):
            part_copy(target_z, offset).wait_recv()
        return [(step,) + relay(step, True), (step,) + relay(step, False)]

    lane = lax.broadcasted_iota(jnp.int32, (chunk, LANES), 1)
    is_first = lane < LANES // 2

    def back(pair, _):
        lanes = lanes_of(pair)
        states = [state_ref[:, lanes]]
        weighted_x = []
        for c in range(chunks):
            rows = pl.ds(c * chunk, chunk)
            to_end = spread_pair(col_ref[pair, rows, :], TO_CHUNK_END, chunk)
            weighted_x.append((x_ref[rows, lanes].astype(F32) * to_end).astype(BF16))
            if c < chunks - 1:
                states.append(
                    states[-1] * row_ref[pair, c + 3 : c + 4, :]
                    + dot(write_t_ref[:, rows], weighted_x[-1], (1, 0))
                )
        skip = row_ref[pair, 0:1, :]
        carry = carry_ref[:, lanes]
        for c in reversed(range(chunks)):
            rows = pl.ds(c * chunk, chunk)
            columns = col_ref[pair, rows, :]
            seg_rows = seg_ref[pair, :, rows]
            x16 = x_ref[rows, lanes]
            x = x16.astype(F32)
            g16 = grad_y_ref[rows, lanes]
            g = g16.astype(F32)
            cross = cross_ref[c]
            state = states[c]
            chunk_exp = row_ref[pair, c + 3 : c + 4, :]
            carry16 = carry.astype(BF16)
            leaving = spread_pair(columns, TO_CHUNK_END, chunk) * dot(
                write_ref[rows, :], carry16, (1, 0)
            )
            halves = []
            summed = None
            for head in range(2):
                decay = chunk_decay(columns, seg_rows, head, chunk)
                mixing = (decay * cross).astype(BF16)
                halves.append(dot(mixing, g16, (0, 0)))
                mask = is_first if head == 0 else jnp.logical_not(is_first)
                pair_dot = dot(jnp.where(mask, g, 0.0).astype(BF16), x16, (1, 1)) * decay
                summed = pair_dot if summed is None else summed + pair_dot
            summed_ref[c] += summed
            grad_x = jnp.where(is_first, halves[0], halves[1]) + leaving
            grad_x_ref[rows, lanes] = (skip * g + grad_x).astype(BF16)
            diff = g * (y_ref[rows, lanes] - skip * x) - x * grad_x
            diff_ref[pair, rows, 0:1] = jnp.sum(
                jnp.where(is_first, diff, 0.0), axis=1, keepdims=True
            )
            diff_ref[pair, rows, 1:2] = jnp.sum(
                jnp.where(is_first, 0.0, diff), axis=1, keepdims=True
            )
            const_ref[pair, c : c + 1, :] = jnp.sum(
                x * leaving, axis=0, keepdims=True
            ) + chunk_exp * jnp.sum(carry * state, axis=0, keepdims=True)
            weighted_g = (g * spread_pair(columns, SEG_EXP, chunk)).astype(BF16)
            map_acc[rows, :LANES] += dot(weighted_x[c], carry16, (1, 1))
            map_acc[rows, LANES:] += dot(weighted_g, state.astype(BF16), (1, 1))
            carry = carry * chunk_exp + dot(read_t_ref[:, rows], weighted_g, (1, 0))
        return 0

    slice_rows = length // tensor

    def slice_of(index):
        return pl.ds(pl.multiple_of(index * slice_rows, 8), slice_rows)

    def scatter(step):
        peer = lax.rem(mine + step, tensor)
        return remote(
            map_acc.at[slice_of(peer)], map_in.at[step - 1],
            (map_sems.at[0, step - 1], map_sems.at[1, step - 1]), "tp", peer,
        )

    def share(step):
        peer = lax.rem(mine + step, tensor)
        return remote(
            grad_map_ref.at[slice_of(mine)], grad_map_ref.at[slice_of(mine)],
            (share_sems.at[0, step - 1], share_sems.at[1, step - 1]), "tp", peer,
        )

    def first_half():
        map_acc[...] = jnp.zeros_like(map_acc)
        summed_ref[...] = jnp.zeros_like(summed_ref)
        for fetch in fetches:
            fetch.wait()
        lax.fori_loop(0, (pairs + 1) // 2, back, 0)

    def second_half():
        lax.fori_loop((pairs + 1) // 2, pairs, back, 0)
        for c in range(chunks):
            rows = pl.ds(c * chunk, chunk)
            summed = summed_ref[c].astype(BF16)
            map_acc[rows, :LANES] += dot(summed, read_ref[rows, :], (0, 0))
            map_acc[rows, LANES:] += dot(summed, write_ref[rows, :], (1, 0))
        for step in range(1, tensor):
            scatter(step).start()

    def reduce_map():
        total = map_acc[slice_of(mine), :]
        for step in range(1, tensor):
            scatter(step).wait_recv()
            total = total + map_in[step - 1]
        grad_map_ref[slice_of(mine), :] = total
        for step in range(1, tensor):
            share(step).start()

    work = [first_half, second_half, reduce_map]
    relays = []
    for step in range(depth - 1):
        relays += serve(step)
        if work:
            work.pop(0)()
    for task in work:
        task()

    for copy in sum_copies:
        copy.wait_recv()
    total = gathered[0]
    for at in range(1, sequence):
        total = total + gathered[at]
    total_ref[...] = total

    for offset in range(1, row):
        part_copy(z, offset).wait_recv()

    def collect(source, at, initial):
        def one(pair, _):
            lanes = lanes_of(pair)
            if initial:
                value = own[z, :, lanes].astype(F32)
                for offset in range(row - 1):
                    value = value + arrived[z, offset, :, lanes].astype(F32)
            else:
                value = acc[:, lanes] + source[at, :, lanes].astype(F32)
            acc[:, lanes] = value
            return 0

        lax.fori_loop(0, pairs, one, 0)

    collect(None, 0, True)
    last_up, last_down = relays[-2][1], relays[-1][1]

    @pl.when(z > 0)
    def _():
        last_up(depth - 2).wait_recv()
        collect(up_in, depth - 2, False)

    @pl.when(z < depth - 1)
    def _():
        last_down(depth - 2).wait_recv()
        collect(down_in, depth - 2, False)

    def turn(pair, _):
        weight_ref[lanes_of(pair), :] = acc[:, lanes_of(pair)].T
        return 0

    lax.fori_loop(0, pairs, turn, 0)

    for step in range(1, tensor):
        share(step).wait_recv()
    for step, copy, is_active in relays:

        @pl.when(is_active)
        def _():
            copy(step).wait_send()

    def sent(step, _):
        for offset in range(1, row):
            part_copy(step, offset).wait_send()
        return 0

    lax.fori_loop(0, depth, sent, 0)
    for half in range(2):
        first, last = bounds[half], bounds[half + 1]
        span = pl.ds(first * LANES, (last - first) * LANES)

        @pl.when(z > 0)
        def _():
            remote(
                chain_out.at[:, span], chain_in.at[:, span],
                (chain_sems.at[0, half], chain_sems.at[1, half]), "seq", me - row,
            ).wait_send()

    for copy in exchanges + sum_copies:
        copy.wait_send()
    for step in range(1, tensor):
        scatter(step).wait_send()
        share(step).wait_send()


def on_device(
    packed_input,
    block_exponent,
    gate_input,
    state_write,
    state_read,
    log_decay,
    skip_weight,
    norm_gain,
    out_weight,
    out_cotangent,
):
    head_count, length = log_decay.shape
    width = packed_input.shape[1]
    states = state_write.shape[1]
    head_width = width // head_count
    pairs = width // LANES
    per_pair = head_count // pairs
    chunk = min(CHUNK, length)
    chunks = length // chunk
    total_width = width * lax.axis_size("tp")
    position = lax.axis_index("seq")
    sequence = lax.axis_size("seq")

    cot_t = lax.all_gather(out_cotangent.T, "tp", axis=0, tiled=True)

    order = jnp.arange(chunk)
    upper = (order[:, None] <= order[None, :]).astype(F32)
    decay_chunks = log_decay.reshape(head_count * chunks, chunk)
    seg = jnp.dot(decay_chunks, upper, precision=PRECISE).reshape(head_count, chunks, chunk)
    chunk_total = seg[:, :, -1]
    chunk_running = jnp.cumsum(chunk_total, axis=1)
    decay_total = chunk_running[:, -1]
    decay_sum = (seg + (chunk_running - chunk_total)[:, :, None]).reshape(head_count, length)
    to_chunk_end = jnp.exp(chunk_total[:, :, None] - seg).reshape(head_count, length)
    seg = seg.reshape(head_count, length)
    to_end = jnp.exp(decay_total[:, None] - decay_sum)
    factor = jnp.exp2(block_exponent.astype(F32))

    flat = jnp.concatenate(
        [factor, seg, jnp.exp(seg), to_chunk_end, jnp.exp(decay_sum), to_end], axis=0
    )
    pair = jnp.arange(pairs)[:, None]
    slot = jnp.arange(COLUMN_COUNT)[None, :]
    of_head = pairs + (slot - 1) // per_pair * head_count + pair * per_pair + (slot - 1) % per_pair
    origin = jnp.where(slot == 0, pair, jnp.where(slot <= 5 * per_pair, of_head, -1))
    picks = (origin.reshape(-1, 1) == jnp.arange(flat.shape[0])[None, :]).astype(F32)
    seg_rows = jnp.dot(picks, flat, precision=PRECISE).reshape(pairs, COLUMN_COUNT, length)
    columns = seg_rows.transpose(0, 2, 1)

    def widen(a):
        return jnp.repeat(a, head_width, axis=-1)

    rows = jnp.stack(
        [widen(skip_weight), norm_gain, jnp.zeros_like(norm_gain)]
        + [widen(jnp.exp(chunk_total[:, c])) for c in range(chunks)],
        axis=0,
    )
    row_count = rows.shape[0]
    rows = rows.reshape(row_count, pairs, LANES).transpose(1, 0, 2)

    totals = lax.all_gather(decay_total[None], "seq", axis=0, tiled=True)
    running = jnp.cumsum(totals, axis=0)
    running_here = lax.dynamic_index_in_dim(running, position, 0, keepdims=False)
    before_here = running_here - decay_total
    sources = jnp.arange(sequence)
    is_earlier = (sources < position)[:, None]
    early = jnp.where(
        is_earlier, jnp.exp(jnp.where(is_earlier, before_here[None] - running, 0.0)), 0.0
    )
    def by_pair(weights):
        return widen(weights).reshape(sequence, pairs, LANES).transpose(1, 0, 2)

    early = by_pair(early)

    write_t, read_t = state_write.T, state_read.T
    cross = lax.dot_general(
        state_read.reshape(chunks, chunk, states),
        state_write.reshape(chunks, chunk, states),
        (((2,), (2,)), ((0,), (0,))),
        preferred_element_type=F32,
    )

    wide_spec = pl.BlockSpec((length, LANES), lambda i: (0, i))
    col_spec = pl.BlockSpec((1, length, COLUMN_COUNT), lambda i: (i, 0, 0))
    seg_spec = pl.BlockSpec((1, COLUMN_COUNT, length), lambda i: (i, 0, 0))
    row_spec = pl.BlockSpec((1, row_count, LANES), lambda i: (i, 0, 0))
    cross_spec = pl.BlockSpec((chunks, chunk, chunk), lambda i: (0, 0, 0))
    map_spec = pl.BlockSpec((length, states), lambda i: (0, 0))
    map_t_spec = pl.BlockSpec((states, length), lambda i: (0, 0))
    state_spec = pl.BlockSpec((states, LANES), lambda i: (0, i))
    piece_spec = pl.BlockSpec((sequence, states, LANES), lambda i: (0, 0, i))
    weight_spec = pl.BlockSpec((1, sequence, LANES), lambda i: (i, 0, 0))
    shape = jax.ShapeDtypeStruct

    def call(kernel, in_specs, out_specs, out_shape, micros):
        return pl.pallas_call(
            kernel,
            grid=(pairs,),
            in_specs=in_specs,
            out_specs=out_specs,
            out_shape=out_shape,
            compiler_params=pltpu.CompilerParams(
                dimension_semantics=("arbitrary",), vmem_limit_bytes=VMEM_LIMIT
            ),
            cost_estimate=pl.CostEstimate(
                flops=int(micros * 9e8), bytes_accessed=int(micros * 1e5), transcendentals=0
            ),
        )

    x, local_state = call(
        unpack_kernel,
        [pl.BlockSpec((length // 8, LANES), lambda i: (0, i)), col_spec, map_t_spec],
        [wide_spec, state_spec],
        [shape((length, width), BF16), shape((states, width), BF16)],
        4,
    )(packed_input, columns, write_t)
    state_pieces = lax.all_gather(local_state[None], "seq", axis=0, tiled=True)

    y_local = call(
        local_kernel,
        [wide_spec, col_spec, seg_spec, row_spec, cross_spec, map_t_spec, map_spec],
        wide_spec,
        shape((length, width), F32),
        10,
    )(x, columns, seg_rows, rows, cross, write_t, state_read)
    grad_v = lax.dot_general(
        cot_t, out_weight, (((0,), (1,)), ((), ())), preferred_element_type=F32
    )

    y_full, state_in, square, inner = call(
        mix_kernel,
        [
            wide_spec, wide_spec, col_spec, row_spec, map_spec, piece_spec, weight_spec,
            wide_spec, wide_spec,
        ],
        [wide_spec, state_spec, map_spec, map_spec],
        [
            shape((length, width), F32),
            shape((states, width), F32),
            shape((length, LANES), F32),
            shape((length, LANES), F32),
        ],
        6,
    )(y_local, x, columns, rows, state_read, state_pieces, early, gate_input, grad_v)
    token_sums = lax.psum(jnp.stack([jnp.sum(square, axis=1), jnp.sum(inner, axis=1)]), "tp")
    scale = lax.rsqrt(token_sums[0] / total_width + 1e-05)
    pull = scale * scale * scale * token_sums[1] / total_width
    scales = jnp.stack([scale, pull], axis=1)

    normed, grad_gate, grad_y, sums, local_cot = call(
        gate_kernel,
        [
            wide_spec, wide_spec, col_spec, row_spec, map_t_spec, wide_spec, wide_spec,
            pl.BlockSpec((length, 2), lambda i: (0, 0)),
        ],
        [
            wide_spec, wide_spec, wide_spec,
            pl.BlockSpec((1, 2, LANES), lambda i: (i, 0, 0)),
            state_spec,
        ],
        [
            shape((length, width), BF16),
            shape((length, width), BF16),
            shape((length, width), BF16),
            shape((pairs, 2, LANES), F32),
            shape((states, width), BF16),
        ],
        6,
    )(y_full, x, columns, rows, read_t, gate_input, grad_v, scales)
    row = chip_rows(sequence)
    depth = sequence // row
    tensor = lax.axis_size("tp")
    cols_out = cot_t.shape[0] // sequence
    decay_row = widen(jnp.exp(decay_total))[None, :]
    vmem = pl.BlockSpec(memory_space=pltpu.VMEM)
    anywhere = pl.BlockSpec(memory_space=pl.ANY)
    block = (cols_out, width)
    dma = pltpu.SemaphoreType.DMA
    hops = depth - 1
    grad_input, grad_map, diff, const, grad_out_weight, totals_out = pl.pallas_call(
        functools.partial(tail_kernel, sequence, tensor),
        in_specs=[vmem] * 13 + [anywhere] * 4,
        out_specs=[vmem] * 6,
        out_shape=[
            shape((length, width), BF16),
            shape((length, 2 * states), F32),
            shape((pairs, length, per_pair), F32),
            shape((pairs, chunks, LANES), F32),
            shape((width, cols_out), F32),
            shape((2, width), F32),
        ],
        scratch_shapes=[
            pltpu.VMEM((depth,) + block, BF16),
            pltpu.VMEM((depth, row - 1) + block, BF16),
            pltpu.VMEM((depth, row - 1) + block, BF16),
            pltpu.VMEM((hops,) + block, BF16),
            pltpu.VMEM((hops,) + block, BF16),
            pltpu.VMEM((hops,) + block, BF16),
            pltpu.VMEM((hops,) + block, BF16),
            pltpu.VMEM(block, F32),
            pltpu.VMEM((row, states, width), BF16),
            pltpu.VMEM((row, 1, width), F32),
            pltpu.VMEM((states, width), BF16),
            pltpu.VMEM((states, width), BF16),
            pltpu.VMEM((states, width), F32),
            pltpu.VMEM((sequence, 2, width), F32),
            pltpu.VMEM((length, 2 * states), F32),
            pltpu.VMEM((tensor - 1, length // tensor, 2 * states), F32),
            pltpu.VMEM((chunks, chunk, chunk), F32),
            pltpu.VMEM((length, width), BF16),
            pltpu.VMEM((length, width), BF16),
            pltpu.VMEM((length, width), F32),
            pltpu.VMEM((pairs, length, COLUMN_COUNT), F32),
            dma((2, depth, row - 1)),
            dma((2, hops)),
            dma((2, hops)),
            dma((2, row - 1)),
            dma((2, row - 1)),
            dma((2, 2)),
            dma((2, sequence - 1)),
            dma((2, tensor - 1)),
            dma((2, tensor - 1)),
            dma((4,)),
        ],
        compiler_params=pltpu.CompilerParams(
            collective_id=1, has_side_effects=True, vmem_limit_bytes=TAIL_VMEM
        ),
        cost_estimate=pl.CostEstimate(
            flops=int(80 * 9e8), bytes_accessed=int(80 * 1e5), transcendentals=0
        ),
    )(
        normed, cot_t, local_cot, decay_row, sums.transpose(1, 0, 2).reshape(2, width), seg_rows,
        rows, cross, state_write, state_read, write_t, read_t, state_in, x, grad_y, y_full, columns,
    )
    grad_gain = totals_out[0]
    grad_skip = jnp.sum(totals_out[1].reshape(head_count, head_width), axis=1)
    grad_write, grad_read = grad_map[:, :states], grad_map[:, states:]
    diff_rows = diff.transpose(0, 2, 1).reshape(head_count * chunks, chunk)
    suffix = jnp.dot(diff_rows, upper.T, precision=PRECISE).reshape(head_count, chunks, chunk)
    const = jnp.sum(const.reshape(pairs, chunks, per_pair, head_width), axis=3)
    const = const.transpose(0, 2, 1).reshape(head_count, chunks)
    grad_decay = (suffix + const[:, :, None]).reshape(head_count, length)
    return (
        grad_input,
        grad_gate,
        grad_write,
        grad_read,
        grad_decay,
        grad_skip,
        grad_gain,
        grad_out_weight,
    )


def solution(mesh):
    placed = (
        P("seq", "tp"),
        P("tp", "seq"),
        P("seq", "tp"),
        P("seq", None),
        P("seq", None),
        P("tp", "seq"),
        P("tp"),
        P("tp"),
        P("tp", None),
        P("seq", "tp"),
    )
    return jax.shard_map(
        on_device,
        mesh=mesh,
        in_specs=placed,
        out_specs=(
            P("seq", "tp"),
            P("seq", "tp"),
            P("seq", None),
            P("seq", None),
            P("tp", "seq"),
            P("tp"),
            P("tp"),
            P("tp", "seq"),
        ),
        check_vma=False,
    )
```

```python
import functools

import jax
import jax.numpy as jnp
from jax import lax
from jax.experimental import pallas as pl
from jax.experimental.pallas import tpu as pltpu
from jax.sharding import PartitionSpec as P

PRECISE = lax.Precision.HIGHEST
F32 = jnp.float32
BF16 = jnp.bfloat16
LANES = 128
CHUNK = 128
VMEM_LIMIT = 48 * 1024 * 1024
PARTS = 2
SITES = ((0, 1), (2, 3), (3, 4), (4, 4))
TAIL_VMEM = 62 * 1024 * 1024
MESH = pl.DeviceIdType.MESH

FACTOR, SEG, SEG_EXP, TO_CHUNK_END, FROM_START, TO_END = 0, 1, 3, 5, 7, 9
COLUMN_COUNT = 16


def dot(a, b, contract):
    return lax.dot_general(a, b, ((contract[:1], contract[1:]), ((), ())), preferred_element_type=F32)


def spread_pair(columns, at, rows):
    lane = lax.broadcasted_iota(jnp.int32, (rows, LANES), 1)
    return jnp.where(lane < LANES // 2, columns[:, at : at + 1], columns[:, at + 1 : at + 2])


def chunk_decay(columns, seg_rows, head, rows):
    token = lax.broadcasted_iota(jnp.int32, (rows, rows), 0)
    source = lax.broadcasted_iota(jnp.int32, (rows, rows), 1)
    spread = columns[:, SEG + head : SEG + head + 1] - seg_rows[SEG + head : SEG + head + 1, :]
    return jnp.exp(jnp.where(token >= source, spread, -1e30))


def chip_rows(sequence):
    return max(d for d in range(1, sequence + 1) if d * d <= sequence and sequence % d == 0)


def visit(z, depth, step):
    low = jnp.minimum(z, depth - 1 - z)
    late = jnp.maximum(step - (depth - 1 - 2 * low), 0)
    half = lax.div(late, 2)
    near = jnp.where(lax.rem(late, 2) == 0, 2 * low - half, half)
    target = jnp.where(step < depth - 1 - 2 * low, depth - 1 - step, near)
    return jnp.where(2 * z <= depth - 1, target, depth - 1 - target)


def lanes_of(pair):
    return pl.ds(pl.multiple_of(pair * LANES, LANES), LANES)


def greet(axes):
    barrier = pltpu.get_barrier_semaphore()
    count = 0
    for axis, size in axes:
        me = lax.axis_index(axis)
        for step in range(1, size):
            pl.semaphore_signal(
                barrier, inc=1, device_id={axis: lax.rem(me + step, size)}, device_id_type=MESH
            )
            count += 1
    pl.semaphore_wait(barrier, count)


def remote(source, target, sems, axis, peer):
    return pltpu.make_async_remote_copy(
        src_ref=source, dst_ref=target, send_sem=sems[0], recv_sem=sems[1],
        device_id={axis: peer}, device_id_type=MESH,
    )


def head_kernel(
    sequence, tensor,
    packed_ref, cot_own, decay_ref, col_ref, seg_ref, row_ref, cross_ref, write_t_ref, read_ref,
    read_t_ref, gate_hbm, weight_hbm,
    x_ref, y_ref, grad_y_ref, normed_ref, grad_gate_ref, sums_ref, cot_state_ref, state_ref, cot_ref,
    grad_v_ref, gate_ref, weight_ref, piece, piece_decay, chain_in, chain_out, square_ref, inner_ref,
    token_ref, scale_ref, pull_ref,
    piece_sems, decay_sems, chain_sems, pair_sems, far_sems, near_sems, token_sems, local_sems,
):
    row = chip_rows(sequence)
    depth = sequence // row
    me = lax.axis_index("seq")
    mine = lax.axis_index("tp")
    z, place = lax.div(me, row), lax.rem(me, row)
    partner = mine + 1 - 2 * lax.rem(mine, 2)
    width = x_ref.shape[1]
    length = x_ref.shape[0]
    pairs = width // LANES
    chunk = min(CHUNK, length)
    chunks = length // chunk
    share = cot_own.shape[0]
    states = read_ref.shape[1]

    fetches = [
        pltpu.make_async_copy(source, target, local_sems.at[i])
        for i, (source, target) in enumerate([(weight_hbm, weight_ref), (gate_hbm, gate_ref)])
    ]
    for fetch in fetches:
        fetch.start()
    greet((("seq", sequence), ("tp", tensor)))

    def part_of(index):
        return cot_ref.at[pl.ds(pl.multiple_of(index * share, 16), share)]

    near = remote(cot_own, part_of(mine), (pair_sems.at[0], pair_sems.at[1]), "tp", partner)
    far = [
        remote(
            cot_own, part_of(mine), (far_sems.at[0, hop - 1], far_sems.at[1, hop - 1]), "tp",
            lax.rem(mine + 2 * hop, tensor),
        )
        for hop in range(1, tensor // 2)
    ]
    for copy in far + [near]:
        copy.start()
    cot_ref[pl.ds(pl.multiple_of(mine * share, 16), share), :] = cot_own[...]

    def neighbour(step):
        return z * row + lax.rem(place + step, row)

    decay_copies = [
        remote(
            decay_ref, piece_decay.at[place],
            (decay_sems.at[0, step - 1], decay_sems.at[1, step - 1]), "seq", neighbour(step),
        )
        for step in range(1, row)
    ]
    for copy in decay_copies:
        copy.start()
    piece_decay[place] = decay_ref[...]

    def unpack(pair, _):
        lanes = lanes_of(pair)
        words = packed_ref[:, lanes]
        groups = words.shape[0]
        wide = jnp.broadcast_to(words[:, None, :], (groups, 8, LANES))
        shifts = 4 * lax.broadcasted_iota(jnp.int32, (groups, 8, LANES), 1)
        fields = jnp.bitwise_and(jnp.right_shift(wide, shifts), 15) - 8
        columns = col_ref[pair]
        x = fields.astype(F32).reshape(length, LANES) * columns[:, FACTOR : FACTOR + 1]
        x_ref[:, lanes] = x.astype(BF16)
        weighted = (x * spread_pair(columns, TO_END, length)).astype(BF16)
        piece[place, :, lanes] = dot(write_t_ref[...], weighted, (1, 0)).astype(BF16)
        return 0

    bounds = [pairs * at // PARTS for at in range(PARTS + 1)]

    def piece_copy(at, step):
        span = pl.ds(bounds[at] * LANES, (bounds[at + 1] - bounds[at]) * LANES)
        return remote(
            piece.at[place, :, span], piece.at[place, :, span],
            (piece_sems.at[0, at, step - 1], piece_sems.at[1, at, step - 1]), "seq", neighbour(step),
        )

    for at in range(PARTS):
        lax.fori_loop(bounds[at], bounds[at + 1], unpack, 0)
        for step in range(1, row):
            piece_copy(at, step).start()

    def hop(at):
        span = pl.ds(bounds[at] * LANES, (bounds[at + 1] - bounds[at]) * LANES)
        return remote(
            chain_out.at[:, span], chain_in.at[:, span],
            (chain_sems.at[0, at], chain_sems.at[1, at]), "seq", me + row,
        )

    def link(at, entering):
        if at == 0:
            for copy in decay_copies:
                copy.wait_recv()
        for step in range(1, row):
            piece_copy(at, step).wait_recv()
        if entering:
            hop(at).wait_recv()

        def one(pair, _):
            lanes = lanes_of(pair)
            group, before = None, jnp.zeros((states, LANES), F32)
            scale, factor = None, jnp.ones((1, LANES), F32)
            for index in range(row):
                term = piece[index, :, lanes].astype(F32)
                decay = piece_decay[index, :, lanes]
                take = index < place
                before = jnp.where(take, term + decay * before, before)
                factor = jnp.where(take, decay * factor, factor)
                group = term if group is None else term + decay * group
                scale = decay if scale is None else decay * scale
            if entering:
                incoming = chain_in[:, lanes].astype(F32)
                group = group + scale * incoming
                before = before + factor * incoming
            state_ref[:, lanes] = before
            chain_out[:, lanes] = group.astype(BF16)
            return 0

        lax.fori_loop(bounds[at], bounds[at + 1], one, 0)

    def visit_chain(site):
        for level in range(min(4, depth)):
            here = [at for at in range(PARTS) if SITES[level][at] == site]
            is_level = z == level if level < 3 else z >= level
            if here:

                @pl.when(is_level)
                def _():
                    for at in here:
                        link(at, level > 0)

                        @pl.when(z < depth - 1)
                        def _():
                            hop(at).start()

    lane = lax.broadcasted_iota(jnp.int32, (chunk, LANES), 1)

    def local(pair, _):
        lanes = lanes_of(pair)
        state = None
        for c in range(chunks):
            part = pl.ds(c * chunk, chunk)
            columns = col_ref[pair, part, :]
            seg_rows = seg_ref[pair, :, part]
            x = x_ref[part, lanes]
            cross = cross_ref[c]
            halves = []
            for head in range(2):
                mixing = (chunk_decay(columns, seg_rows, head, chunk) * cross).astype(BF16)
                halves.append(dot(mixing, x, (1, 0)))
            y = jnp.where(lane < LANES // 2, halves[0], halves[1])
            if state is not None:
                y = y + spread_pair(columns, SEG_EXP, chunk) * dot(
                    read_ref[part, :], state.astype(BF16), (1, 0)
                )
            y_ref[part, lanes] = y
            if c < chunks - 1:
                weighted = (x.astype(F32) * spread_pair(columns, TO_CHUNK_END, chunk)).astype(BF16)
                added = dot(write_t_ref[:, part], weighted, (1, 0))
                state = (
                    added if state is None else state * row_ref[pair, c + 3 : c + 4, :] + added
                )
        return 0

    third, most = pairs // 3, 3 * pairs // 4
    lax.fori_loop(0, third, local, 0)
    visit_chain(0)
    lax.fori_loop(third, most, local, 0)
    visit_chain(1)
    lax.fori_loop(most, pairs, local, 0)
    visit_chain(2)

    forwards = []
    for index, copy in enumerate(far):
        copy.wait_recv()
        source = lax.rem(mine + tensor - 2 * (index + 1), tensor)
        forwards.append(
            remote(
                part_of(source), part_of(source), (near_sems.at[0, index], near_sems.at[1, index]),
                "tp", partner,
            )
        )
        forwards[-1].start()
    near.wait_recv()
    for fetch in fetches:
        fetch.wait()
    for copy in forwards:
        copy.wait_recv()

    def pull_back(first, last):
        rows = pl.ds(first * LANES, (last - first) * LANES)
        block = dot(weight_ref[rows, :], cot_ref[...], (1, 0))
        for pair in range(first, last):
            at = (pair - first) * LANES
            grad_v_ref[:, pair * LANES : (pair + 1) * LANES] = block[at : at + LANES, :].T

    pull_back(0, pairs // 2)
    visit_chain(3)
    pull_back(pairs // 2, pairs)
    visit_chain(4)

    square_ref[...] = jnp.zeros_like(square_ref)
    inner_ref[...] = jnp.zeros_like(inner_ref)

    def mix(pair, _):
        lanes = lanes_of(pair)
        carried = dot(read_ref[...], state_ref[:, lanes].astype(BF16), (1, 0))
        y = (
            y_ref[:, lanes]
            + spread_pair(col_ref[pair], FROM_START, length) * carried
            + row_ref[pair, 0:1, :] * x_ref[:, lanes].astype(F32)
        )
        y_ref[:, lanes] = y
        gate = gate_ref[:, lanes].astype(F32)
        mixed = y * gate * jax.nn.sigmoid(gate)
        square_ref[...] += mixed * mixed
        inner_ref[...] += grad_v_ref[:, lanes] * row_ref[pair, 1:2, :] * mixed
        return 0

    lax.fori_loop(0, pairs, mix, 0)
    token_ref[0, 0:1, :] = jnp.sum(square_ref[...].T, axis=0, keepdims=True)
    token_ref[0, 1:2, :] = jnp.sum(inner_ref[...].T, axis=0, keepdims=True)
    token_copies = [
        remote(
            token_ref.at[0], token_ref.at[step],
            (token_sems.at[0, step - 1], token_sems.at[1, step - 1]), "tp",
            lax.rem(mine + step, tensor),
        )
        for step in range(1, tensor)
    ]
    for copy in token_copies:
        copy.start()
    for copy in token_copies:
        copy.wait_recv()
    token = token_ref[0]
    for step in range(1, tensor):
        token = token + token_ref[step]
    scale = lax.rsqrt(token[0:1, :] / (width * tensor) + 1e-05)
    pull = scale * scale * scale * token[1:2, :] / (width * tensor)
    scale_ref[...] = jnp.broadcast_to(scale, (LANES, length)).T
    pull_ref[...] = jnp.broadcast_to(pull, (LANES, length)).T

    def shape_gate(pair, _):
        lanes = lanes_of(pair)
        gain = row_ref[pair, 1:2, :]
        y = y_ref[:, lanes]
        gate = gate_ref[:, lanes].astype(F32)
        sigma = jax.nn.sigmoid(gate)
        active = gate * sigma
        mixed = y * active
        mixed_scaled = mixed * scale_ref[...]
        normed_ref[:, lanes] = (mixed_scaled * gain).astype(BF16)
        grad_v = grad_v_ref[:, lanes]
        grad_mixed = scale_ref[...] * grad_v * gain - mixed * pull_ref[...]
        grad_gate_ref[:, lanes] = (
            grad_mixed * y * sigma * (1.0 + gate * (1.0 - sigma))
        ).astype(BF16)
        grad_y = grad_mixed * active
        grad_y_ref[:, lanes] = grad_y.astype(BF16)
        sums_ref[0:1, lanes] = jnp.sum(grad_v * mixed_scaled, axis=0, keepdims=True)
        sums_ref[1:2, lanes] = jnp.sum(grad_y * x_ref[:, lanes].astype(F32), axis=0, keepdims=True)
        weighted = (grad_y * spread_pair(col_ref[pair], FROM_START, length)).astype(BF16)
        cot_state_ref[:, lanes] = dot(read_t_ref[...], weighted, (1, 0)).astype(BF16)
        return 0

    lax.fori_loop(0, pairs, shape_gate, 0)

    for copy in far + [near] + forwards + decay_copies + token_copies:
        copy.wait_send()
    for at in range(PARTS):
        for step in range(1, row):
            piece_copy(at, step).wait_send()

        @pl.when(z < depth - 1)
        def _():
            hop(at).wait_send()


def tail_kernel(
    sequence, tensor,
    normed_ref, cot_ref, local_ref, decay_ref, sums_ref, seg_ref, row_ref, cross_ref, write_ref,
    read_ref, write_t_ref, read_t_ref, state_ref, x_hbm, grad_y_hbm, y_hbm, col_hbm,
    grad_x_ref, grad_map_ref, diff_ref, const_ref, weight_ref, total_ref,
    own, part, arrived, up_out, up_in, down_out, down_in, acc, piece, piece_decay, chain_in,
    chain_out, carry_ref, gathered, map_acc, map_in, summed_ref, x_ref, grad_y_ref, y_ref, col_ref,
    part_sems, up_sems, down_sems, piece_sems, decay_sems, chain_sems, sum_sems, map_sems, share_sems,
    local_sems,
):
    row = chip_rows(sequence)
    depth = sequence // row
    me = lax.axis_index("seq")
    mine = lax.axis_index("tp")
    z, place = lax.div(me, row), lax.rem(me, row)
    length, width = normed_ref.shape
    pairs = width // LANES
    columns_out = weight_ref.shape[1]
    chunk = min(CHUNK, length)
    chunks = length // chunk

    fetches = [
        pltpu.make_async_copy(source, target, local_sems.at[i])
        for i, (source, target) in enumerate(
            [(x_hbm, x_ref), (grad_y_hbm, grad_y_ref), (y_hbm, y_ref), (col_hbm, col_ref)]
        )
    ]
    for fetch in fetches:
        fetch.start()
    greet((("seq", sequence), ("tp", tensor)))

    def neighbour(step):
        return z * row + lax.rem(place + step, row)

    exchanges = []
    for step in range(1, row):
        exchanges.append(
            remote(
                local_ref, piece.at[place],
                (piece_sems.at[0, step - 1], piece_sems.at[1, step - 1]), "seq", neighbour(step),
            )
        )
        exchanges.append(
            remote(
                decay_ref, piece_decay.at[place],
                (decay_sems.at[0, step - 1], decay_sems.at[1, step - 1]), "seq", neighbour(step),
            )
        )
    sum_copies = [
        remote(
            sums_ref, gathered.at[me], (sum_sems.at[0, step - 1], sum_sems.at[1, step - 1]), "seq",
            lax.rem(me + step, sequence),
        )
        for step in range(1, sequence)
    ]
    for copy in exchanges + sum_copies:
        copy.start()
    piece[place] = local_ref[...]
    piece_decay[place] = decay_ref[...]
    gathered[me] = sums_ref[...]

    def part_copy(target_z, step):
        return remote(
            part.at[target_z, step - 1], arrived.at[target_z, step - 1],
            (part_sems.at[0, target_z, step - 1], part_sems.at[1, target_z, step - 1]), "seq",
            neighbour(step),
        )

    def multiply(step, _):
        target_z = visit(z, depth, step)
        for offset in list(range(1, row)) + [0]:
            block = target_z * row + lax.rem(place + offset, row)
            taken = cot_ref[pl.ds(pl.multiple_of(block * columns_out, 16), columns_out), :]
            for at in range(0, width, 2 * LANES):
                span = pl.ds(at, min(2 * LANES, width - at))
                product = dot(taken, normed_ref[:, span], (1, 0)).astype(BF16)
                if offset:
                    part[target_z, offset - 1, :, span] = product
                else:
                    own[target_z, :, span] = product
            if offset:
                part_copy(target_z, offset).start()
        return 0

    lax.fori_loop(0, depth, multiply, 0)

    for copy in exchanges:
        copy.wait_recv()
    bounds = [0, (pairs + 1) // 2, pairs]
    for half in range(2):
        first, last = bounds[half], bounds[half + 1]
        span = pl.ds(first * LANES, (last - first) * LANES)
        hop = remote(
            chain_out.at[:, span], chain_in.at[:, span],
            (chain_sems.at[0, half], chain_sems.at[1, half]), "seq", me - row,
        )

        def link(entering):
            def one(pair, _):
                lanes = lanes_of(pair)
                group, after = None, jnp.zeros((piece.shape[1], LANES), F32)
                scale, factor = None, jnp.ones((1, LANES), F32)
                for at in reversed(range(row)):
                    term = piece[at, :, lanes].astype(F32)
                    decay = piece_decay[at, :, lanes]
                    take = at > place
                    after = jnp.where(take, term + decay * after, after)
                    factor = jnp.where(take, decay * factor, factor)
                    group = term if group is None else term + decay * group
                    scale = decay if scale is None else decay * scale
                if entering:
                    incoming = chain_in[:, lanes].astype(F32)
                    group = group + scale * incoming
                    after = after + factor * incoming
                carry_ref[:, lanes] = after
                chain_out[:, lanes] = group.astype(BF16)
                return 0

            lax.fori_loop(first, last, one, 0)

        @pl.when(z == depth - 1)
        def _():
            link(False)

        @pl.when(z < depth - 1)
        def _():
            hop.wait_recv()
            link(True)

        @pl.when(z > 0)
        def _():
            hop.start()

    def relay(step, up):
        target_z = z + (depth - 1 - step) if up else z - (depth - 1) + step
        outgoing, incoming, sems = (up_out, up_in, up_sems) if up else (down_out, down_in, down_sems)
        is_end = z == 0 if up else z == depth - 1
        is_active = z <= step if up else z >= depth - 1 - step

        def copy(at):
            return remote(
                outgoing.at[at], incoming.at[at], (sems.at[0, at], sems.at[1, at]), "seq",
                me + row if up else me - row,
            )

        def add(more):
            def one(pair, _):
                lanes = lanes_of(pair)
                value = own[target_z, :, lanes].astype(F32)
                for at in range(row - 1):
                    value = value + arrived[target_z, at, :, lanes].astype(F32)
                if more:
                    value = value + incoming[step - 1, :, lanes].astype(F32)
                outgoing[step, :, lanes] = value.astype(BF16)
                return 0

            lax.fori_loop(0, pairs, one, 0)

        @pl.when(is_end)
        def _():
            add(False)

        if step > 0:

            @pl.when(jnp.logical_and(is_active, jnp.logical_not(is_end)))
            def _():
                copy(step - 1).wait_recv()
                add(True)

        @pl.when(is_active)
        def _():
            copy(step).start()

        return copy, is_active

    def serve(step):
        target_z = visit(z, depth, step)
        for offset in range(1, row):
            part_copy(target_z, offset).wait_recv()
        return [(step,) + relay(step, True), (step,) + relay(step, False)]

    lane = lax.broadcasted_iota(jnp.int32, (chunk, LANES), 1)
    is_first = lane < LANES // 2

    def back(pair, _):
        lanes = lanes_of(pair)
        states = [state_ref[:, lanes]]
        weighted_x = []
        for c in range(chunks):
            rows = pl.ds(c * chunk, chunk)
            to_end = spread_pair(col_ref[pair, rows, :], TO_CHUNK_END, chunk)
            weighted_x.append((x_ref[rows, lanes].astype(F32) * to_end).astype(BF16))
            if c < chunks - 1:
                states.append(
                    states[-1] * row_ref[pair, c + 3 : c + 4, :]
                    + dot(write_t_ref[:, rows], weighted_x[-1], (1, 0))
                )
        skip = row_ref[pair, 0:1, :]
        carry = carry_ref[:, lanes]
        for c in reversed(range(chunks)):
            rows = pl.ds(c * chunk, chunk)
            columns = col_ref[pair, rows, :]
            seg_rows = seg_ref[pair, :, rows]
            x16 = x_ref[rows, lanes]
            x = x16.astype(F32)
            g16 = grad_y_ref[rows, lanes]
            g = g16.astype(F32)
            cross = cross_ref[c]
            state = states[c]
            chunk_exp = row_ref[pair, c + 3 : c + 4, :]
            carry16 = carry.astype(BF16)
            leaving = spread_pair(columns, TO_CHUNK_END, chunk) * dot(
                write_ref[rows, :], carry16, (1, 0)
            )
            halves = []
            summed = None
            for head in range(2):
                decay = chunk_decay(columns, seg_rows, head, chunk)
                mixing = (decay * cross).astype(BF16)
                halves.append(dot(mixing, g16, (0, 0)))
                mask = is_first if head == 0 else jnp.logical_not(is_first)
                pair_dot = dot(jnp.where(mask, g, 0.0).astype(BF16), x16, (1, 1)) * decay
                summed = pair_dot if summed is None else summed + pair_dot
            summed_ref[c] += summed
            grad_x = jnp.where(is_first, halves[0], halves[1]) + leaving
            grad_x_ref[rows, lanes] = (skip * g + grad_x).astype(BF16)
            diff = g * (y_ref[rows, lanes] - skip * x) - x * grad_x
            diff_ref[pair, rows, 0:1] = jnp.sum(
                jnp.where(is_first, diff, 0.0), axis=1, keepdims=True
            )
            diff_ref[pair, rows, 1:2] = jnp.sum(
                jnp.where(is_first, 0.0, diff), axis=1, keepdims=True
            )
            const_ref[pair, c : c + 1, :] = jnp.sum(
                x * leaving, axis=0, keepdims=True
            ) + chunk_exp * jnp.sum(carry * state, axis=0, keepdims=True)
            weighted_g = (g * spread_pair(columns, SEG_EXP, chunk)).astype(BF16)
            map_acc[rows, :LANES] += dot(weighted_x[c], carry16, (1, 1))
            map_acc[rows, LANES:] += dot(weighted_g, state.astype(BF16), (1, 1))
            carry = carry * chunk_exp + dot(read_t_ref[:, rows], weighted_g, (1, 0))
        return 0

    slice_rows = length // tensor

    def slice_of(index):
        return pl.ds(pl.multiple_of(index * slice_rows, 8), slice_rows)

    def scatter(step):
        peer = lax.rem(mine + step, tensor)
        return remote(
            map_acc.at[slice_of(peer)], map_in.at[step - 1],
            (map_sems.at[0, step - 1], map_sems.at[1, step - 1]), "tp", peer,
        )

    def share(step):
        peer = lax.rem(mine + step, tensor)
        return remote(
            grad_map_ref.at[slice_of(mine)], grad_map_ref.at[slice_of(mine)],
            (share_sems.at[0, step - 1], share_sems.at[1, step - 1]), "tp", peer,
        )

    def first_half():
        map_acc[...] = jnp.zeros_like(map_acc)
        summed_ref[...] = jnp.zeros_like(summed_ref)
        for fetch in fetches:
            fetch.wait()
        lax.fori_loop(0, (pairs + 1) // 2, back, 0)

    def second_half():
        lax.fori_loop((pairs + 1) // 2, pairs, back, 0)
        for c in range(chunks):
            rows = pl.ds(c * chunk, chunk)
            summed = summed_ref[c].astype(BF16)
            map_acc[rows, :LANES] += dot(summed, read_ref[rows, :], (0, 0))
            map_acc[rows, LANES:] += dot(summed, write_ref[rows, :], (1, 0))
        for step in range(1, tensor):
            scatter(step).start()

    def reduce_map():
        total = map_acc[slice_of(mine), :]
        for step in range(1, tensor):
            scatter(step).wait_recv()
            total = total + map_in[step - 1]
        grad_map_ref[slice_of(mine), :] = total
        for step in range(1, tensor):
            share(step).start()

    work = [first_half, second_half, reduce_map]
    relays = []
    for step in range(depth - 1):
        relays += serve(step)
        if work:
            work.pop(0)()
    for task in work:
        task()

    for copy in sum_copies:
        copy.wait_recv()
    total = gathered[0]
    for at in range(1, sequence):
        total = total + gathered[at]
    total_ref[...] = total

    for offset in range(1, row):
        part_copy(z, offset).wait_recv()

    def collect(source, at, initial):
        def one(pair, _):
            lanes = lanes_of(pair)
            if initial:
                value = own[z, :, lanes].astype(F32)
                for offset in range(row - 1):
                    value = value + arrived[z, offset, :, lanes].astype(F32)
            else:
                value = acc[:, lanes] + source[at, :, lanes].astype(F32)
            acc[:, lanes] = value
            return 0

        lax.fori_loop(0, pairs, one, 0)

    collect(None, 0, True)
    last_up, last_down = relays[-2][1], relays[-1][1]

    @pl.when(z > 0)
    def _():
        last_up(depth - 2).wait_recv()
        collect(up_in, depth - 2, False)

    @pl.when(z < depth - 1)
    def _():
        last_down(depth - 2).wait_recv()
        collect(down_in, depth - 2, False)

    def turn(pair, _):
        weight_ref[lanes_of(pair), :] = acc[:, lanes_of(pair)].T
        return 0

    lax.fori_loop(0, pairs, turn, 0)

    for step in range(1, tensor):
        share(step).wait_recv()
    for step, copy, is_active in relays:

        @pl.when(is_active)
        def _():
            copy(step).wait_send()

    def sent(step, _):
        for offset in range(1, row):
            part_copy(step, offset).wait_send()
        return 0

    lax.fori_loop(0, depth, sent, 0)
    for half in range(2):
        first, last = bounds[half], bounds[half + 1]
        span = pl.ds(first * LANES, (last - first) * LANES)

        @pl.when(z > 0)
        def _():
            remote(
                chain_out.at[:, span], chain_in.at[:, span],
                (chain_sems.at[0, half], chain_sems.at[1, half]), "seq", me - row,
            ).wait_send()

    for copy in exchanges + sum_copies:
        copy.wait_send()
    for step in range(1, tensor):
        scatter(step).wait_send()
        share(step).wait_send()


def on_device(
    packed_input,
    block_exponent,
    gate_input,
    state_write,
    state_read,
    log_decay,
    skip_weight,
    norm_gain,
    out_weight,
    out_cotangent,
):
    head_count, length = log_decay.shape
    width = packed_input.shape[1]
    states = state_write.shape[1]
    head_width = width // head_count
    pairs = width // LANES
    per_pair = head_count // pairs
    chunk = min(CHUNK, length)
    chunks = length // chunk
    sequence = lax.axis_size("seq")

    order = jnp.arange(chunk)
    upper = (order[:, None] <= order[None, :]).astype(F32)
    decay_chunks = log_decay.reshape(head_count * chunks, chunk)
    seg = jnp.dot(decay_chunks, upper, precision=PRECISE).reshape(head_count, chunks, chunk)
    chunk_total = seg[:, :, -1]
    chunk_running = jnp.cumsum(chunk_total, axis=1)
    decay_total = chunk_running[:, -1]
    decay_sum = (seg + (chunk_running - chunk_total)[:, :, None]).reshape(head_count, length)
    to_chunk_end = jnp.exp(chunk_total[:, :, None] - seg).reshape(head_count, length)
    seg = seg.reshape(head_count, length)
    to_end = jnp.exp(decay_total[:, None] - decay_sum)
    factor = jnp.exp2(block_exponent.astype(F32))

    flat = jnp.concatenate(
        [factor, seg, jnp.exp(seg), to_chunk_end, jnp.exp(decay_sum), to_end], axis=0
    )
    pair = jnp.arange(pairs)[:, None]
    slot = jnp.arange(COLUMN_COUNT)[None, :]
    of_head = pairs + (slot - 1) // per_pair * head_count + pair * per_pair + (slot - 1) % per_pair
    origin = jnp.where(slot == 0, pair, jnp.where(slot <= 5 * per_pair, of_head, -1))
    picks = (origin.reshape(-1, 1) == jnp.arange(flat.shape[0])[None, :]).astype(F32)
    seg_rows = jnp.dot(picks, flat, precision=PRECISE).reshape(pairs, COLUMN_COUNT, length)
    columns = seg_rows.transpose(0, 2, 1)

    def widen(a):
        return jnp.repeat(a, head_width, axis=-1)

    rows = jnp.stack(
        [widen(skip_weight), norm_gain, jnp.zeros_like(norm_gain)]
        + [widen(jnp.exp(chunk_total[:, c])) for c in range(chunks)],
        axis=0,
    )
    row_count = rows.shape[0]
    rows = rows.reshape(row_count, pairs, LANES).transpose(1, 0, 2)

    write_t, read_t = state_write.T, state_read.T
    cross = lax.dot_general(
        state_read.reshape(chunks, chunk, states),
        state_write.reshape(chunks, chunk, states),
        (((2,), (2,)), ((0,), (0,))),
        preferred_element_type=F32,
    )

    shape = jax.ShapeDtypeStruct
    vmem = pl.BlockSpec(memory_space=pltpu.VMEM)
    anywhere = pl.BlockSpec(memory_space=pl.ANY)
    dma = pltpu.SemaphoreType.DMA
    row = chip_rows(sequence)
    depth = sequence // row
    tensor = lax.axis_size("tp")
    decay_row = widen(jnp.exp(decay_total))[None, :]
    cot_own = out_cotangent.T
    model = cot_own.shape[0] * tensor
    x, y_full, grad_y, normed, grad_gate, sums, local_cot, state_in, cot_t = pl.pallas_call(
        functools.partial(head_kernel, sequence, tensor),
        in_specs=[vmem] * 10 + [anywhere] * 2,
        out_specs=[vmem] * 9,
        out_shape=[
            shape((length, width), BF16),
            shape((length, width), F32),
            shape((length, width), BF16),
            shape((length, width), BF16),
            shape((length, width), BF16),
            shape((2, width), F32),
            shape((states, width), BF16),
            shape((states, width), F32),
            shape((model, length), BF16),
        ],
        scratch_shapes=[
            pltpu.VMEM((length, width), F32),
            pltpu.VMEM((length, width), BF16),
            pltpu.VMEM((width, model), BF16),
            pltpu.VMEM((row, states, width), BF16),
            pltpu.VMEM((row, 1, width), F32),
            pltpu.VMEM((states, width), BF16),
            pltpu.VMEM((states, width), BF16),
            pltpu.VMEM((length, LANES), F32),
            pltpu.VMEM((length, LANES), F32),
            pltpu.VMEM((tensor, 2, length), F32),
            pltpu.VMEM((length, LANES), F32),
            pltpu.VMEM((length, LANES), F32),
            dma((2, PARTS, row - 1)),
            dma((2, row - 1)),
            dma((2, PARTS)),
            dma((2,)),
            dma((2, tensor // 2 - 1)),
            dma((2, tensor // 2 - 1)),
            dma((2, tensor - 1)),
            dma((2,)),
        ],
        compiler_params=pltpu.CompilerParams(
            collective_id=2, has_side_effects=True, vmem_limit_bytes=TAIL_VMEM
        ),
        cost_estimate=pl.CostEstimate(
            flops=int(50 * 9e8), bytes_accessed=int(50 * 1e5), transcendentals=0
        ),
    )(
        packed_input, cot_own, decay_row, columns, seg_rows, rows, cross, write_t, state_read, read_t,
        gate_input, out_weight,
    )

    cols_out = cot_t.shape[0] // sequence
    block = (cols_out, width)
    hops = depth - 1
    grad_input, grad_map, diff, const, grad_out_weight, totals_out = pl.pallas_call(
        functools.partial(tail_kernel, sequence, tensor),
        in_specs=[vmem] * 13 + [anywhere] * 4,
        out_specs=[vmem] * 6,
        out_shape=[
            shape((length, width), BF16),
            shape((length, 2 * states), F32),
            shape((pairs, length, per_pair), F32),
            shape((pairs, chunks, LANES), F32),
            shape((width, cols_out), F32),
            shape((2, width), F32),
        ],
        scratch_shapes=[
            pltpu.VMEM((depth,) + block, BF16),
            pltpu.VMEM((depth, row - 1) + block, BF16),
            pltpu.VMEM((depth, row - 1) + block, BF16),
            pltpu.VMEM((hops,) + block, BF16),
            pltpu.VMEM((hops,) + block, BF16),
            pltpu.VMEM((hops,) + block, BF16),
            pltpu.VMEM((hops,) + block, BF16),
            pltpu.VMEM(block, F32),
            pltpu.VMEM((row, states, width), BF16),
            pltpu.VMEM((row, 1, width), F32),
            pltpu.VMEM((states, width), BF16),
            pltpu.VMEM((states, width), BF16),
            pltpu.VMEM((states, width), F32),
            pltpu.VMEM((sequence, 2, width), F32),
            pltpu.VMEM((length, 2 * states), F32),
            pltpu.VMEM((tensor - 1, length // tensor, 2 * states), F32),
            pltpu.VMEM((chunks, chunk, chunk), F32),
            pltpu.VMEM((length, width), BF16),
            pltpu.VMEM((length, width), BF16),
            pltpu.VMEM((length, width), F32),
            pltpu.VMEM((pairs, length, COLUMN_COUNT), F32),
            dma((2, depth, row - 1)),
            dma((2, hops)),
            dma((2, hops)),
            dma((2, row - 1)),
            dma((2, row - 1)),
            dma((2, 2)),
            dma((2, sequence - 1)),
            dma((2, tensor - 1)),
            dma((2, tensor - 1)),
            dma((4,)),
        ],
        compiler_params=pltpu.CompilerParams(
            collective_id=1, has_side_effects=True, vmem_limit_bytes=TAIL_VMEM
        ),
        cost_estimate=pl.CostEstimate(
            flops=int(80 * 9e8), bytes_accessed=int(80 * 1e5), transcendentals=0
        ),
    )(
        normed, cot_t, local_cot, decay_row, sums, seg_rows,
        rows, cross, state_write, state_read, write_t, read_t, state_in, x, grad_y, y_full, columns,
    )
    grad_gain = totals_out[0]
    grad_skip = jnp.sum(totals_out[1].reshape(head_count, head_width), axis=1)
    grad_write, grad_read = grad_map[:, :states], grad_map[:, states:]
    diff_rows = diff.transpose(0, 2, 1).reshape(head_count * chunks, chunk)
    suffix = jnp.dot(diff_rows, upper.T, precision=PRECISE).reshape(head_count, chunks, chunk)
    const = jnp.sum(const.reshape(pairs, chunks, per_pair, head_width), axis=3)
    const = const.transpose(0, 2, 1).reshape(head_count, chunks)
    grad_decay = (suffix + const[:, :, None]).reshape(head_count, length)
    return (
        grad_input,
        grad_gate,
        grad_write,
        grad_read,
        grad_decay,
        grad_skip,
        grad_gain,
        grad_out_weight,
    )


def solution(mesh):
    placed = (
        P("seq", "tp"),
        P("tp", "seq"),
        P("seq", "tp"),
        P("seq", None),
        P("seq", None),
        P("tp", "seq"),
        P("tp"),
        P("tp"),
        P("tp", None),
        P("seq", "tp"),
    )
    return jax.shard_map(
        on_device,
        mesh=mesh,
        in_specs=placed,
        out_specs=(
            P("seq", "tp"),
            P("seq", "tp"),
            P("seq", None),
            P("seq", None),
            P("tp", "seq"),
            P("tp"),
            P("tp"),
            P("tp", "seq"),
        ),
        check_vma=False,
    )
```

```python
import functools

import jax
import jax.numpy as jnp
from jax import lax
from jax.experimental import pallas as pl
from jax.experimental.pallas import tpu as pltpu
from jax.sharding import PartitionSpec as P

PRECISE = lax.Precision.HIGHEST
F32 = jnp.float32
BF16 = jnp.bfloat16
LANES = 128
CHUNK = 128
PARTS = 2
SITES = ((0, 1), (2, 3), (3, 4), (4, 4))
LAYER_VMEM = 67043328
MESH = pl.DeviceIdType.MESH

FACTOR, SEG, SEG_EXP, TO_CHUNK_END, FROM_START, TO_END = 0, 1, 3, 5, 7, 9
COLUMN_COUNT = 16


def dot(a, b, contract):
    return lax.dot_general(a, b, ((contract[:1], contract[1:]), ((), ())), preferred_element_type=F32)


def precise_dot(a, b, contract):
    return lax.dot_general(
        a, b, ((contract[:1], contract[1:]), ((), ())), precision=PRECISE, preferred_element_type=F32
    )


def spread_pair(columns, at, rows):
    lane = lax.broadcasted_iota(jnp.int32, (rows, LANES), 1)
    return jnp.where(lane < LANES // 2, columns[:, at : at + 1], columns[:, at + 1 : at + 2])


def chunk_decay(columns, seg_rows, head, rows):
    token = lax.broadcasted_iota(jnp.int32, (rows, rows), 0)
    source = lax.broadcasted_iota(jnp.int32, (rows, rows), 1)
    spread = columns[:, SEG + head : SEG + head + 1] - seg_rows[SEG + head : SEG + head + 1, :]
    return jnp.exp(jnp.where(token >= source, spread, -1e30))


def chip_rows(sequence):
    return max(d for d in range(1, sequence + 1) if d * d <= sequence and sequence % d == 0)


def visit(z, depth, step):
    low = jnp.minimum(z, depth - 1 - z)
    late = jnp.maximum(step - (depth - 1 - 2 * low), 0)
    half = lax.div(late, 2)
    near = jnp.where(lax.rem(late, 2) == 0, 2 * low - half, half)
    target = jnp.where(step < depth - 1 - 2 * low, depth - 1 - step, near)
    return jnp.where(2 * z <= depth - 1, target, depth - 1 - target)


def lanes_of(pair):
    return pl.ds(pl.multiple_of(pair * LANES, LANES), LANES)


def greet(axes):
    barrier = pltpu.get_barrier_semaphore()
    count = 0
    for axis, size in axes:
        me = lax.axis_index(axis)
        for step in range(1, size):
            pl.semaphore_signal(
                barrier, inc=1, device_id={axis: lax.rem(me + step, size)}, device_id_type=MESH
            )
            count += 1
    pl.semaphore_wait(barrier, count)


def remote(source, target, sems, axis, peer):
    return pltpu.make_async_remote_copy(
        src_ref=source, dst_ref=target, send_sem=sems[0], recv_sem=sems[1],
        device_id={axis: peer}, device_id_type=MESH,
    )


def layer_kernel(
    sequence, tensor,
    packed_ref, exponent_ref, log_ref, skip_ref, gain_ref, write_ref, read_ref, cot_in, gate_hbm,
    weight_hbm,
    grad_x_hbm, grad_gate_hbm, grad_write_ref, grad_read_ref, grad_decay_ref, weight_out, total_ref,
    x_ref, y_ref, grad_y_ref, normed_ref, grad_gate_ref, grad_x_ref, sums_ref, state_ref, cot_ref,
    cot_own, col_ref, seg_ref, flat_ref, cross_ref, write_t_ref, read_t_ref,
    grad_v_ref, gate_ref, weight_ref, piece, piece_decay, chain_in, chain_out, square_ref, inner_ref,
    token_ref, scale_ref, pull_ref,
    piece_sems, decay_sems, chain_sems, pair_sems, far_sems, near_sems, token_sems, local_sems,
    own, part, arrived, up_out, up_in, down_out, down_in, acc, back_piece, back_in,
    back_out, carry_ref, gathered, map_acc, map_in, map_sum, summed_ref, diff_ref, diff_rows, const_ref,
    part_sems, up_sems, down_sems, back_sems, link_sems, sum_sems, map_sems, share_sems, store_sems,
):
    row = chip_rows(sequence)
    depth = sequence // row
    me = lax.axis_index("seq")
    mine = lax.axis_index("tp")
    z, place = lax.div(me, row), lax.rem(me, row)
    partner = mine + 1 - 2 * lax.rem(mine, 2)
    width = x_ref.shape[1]
    length = x_ref.shape[0]
    pairs = width // LANES
    chunk = min(CHUNK, length)
    chunks = length // chunk
    share = cot_own.shape[0]
    states = read_ref.shape[1]
    columns_out = weight_out.shape[1]

    fetches = [
        pltpu.make_async_copy(source, target, local_sems.at[i])
        for i, (source, target) in enumerate([(weight_hbm, weight_ref), (gate_hbm, gate_ref)])
    ]
    for fetch in fetches:
        fetch.start()
    for at in range(0, share, LANES):
        wide = min(LANES, share - at)
        cot_own[at : at + wide, :] = cot_in[:, at : at + wide].astype(F32).T.astype(BF16)
    greet((("seq", sequence), ("tp", tensor)))

    def part_of(index):
        return cot_ref.at[pl.ds(pl.multiple_of(index * share, 16), share)]

    near = remote(cot_own, part_of(mine), (pair_sems.at[0], pair_sems.at[1]), "tp", partner)
    far = [
        remote(
            cot_own, part_of(mine), (far_sems.at[0, hop - 1], far_sems.at[1, hop - 1]), "tp",
            lax.rem(mine + 2 * hop, tensor),
        )
        for hop in range(1, tensor // 2)
    ]
    for copy in far + [near]:
        copy.start()
    cot_ref[pl.ds(pl.multiple_of(mine * share, 16), share), :] = cot_own[...]

    def neighbour(step):
        return z * row + lax.rem(place + step, row)

    decay_copies = [
        remote(
            piece_decay.at[place], piece_decay.at[place],
            (decay_sems.at[0, step - 1], decay_sems.at[1, step - 1]), "seq", neighbour(step),
        )
        for step in range(1, row)
    ]

    def skip_row(pair):
        lanes = lax.broadcasted_iota(jnp.int32, (1, LANES), 1)
        return jnp.where(lanes < LANES // 2, skip_ref[2 * pair], skip_ref[2 * pair + 1])

    def chunk_scale(pair, c):
        return spread_pair(col_ref[pair, (c + 1) * chunk - 1 : (c + 1) * chunk, :], SEG_EXP, 1)

    heads = log_ref.shape[0]
    order = lax.broadcasted_iota(jnp.int32, (chunk, chunk), 0)
    other = lax.broadcasted_iota(jnp.int32, (chunk, chunk), 1)
    upper = jnp.where(order <= other, 1.0, 0.0)
    lower = jnp.where(order >= other, 1.0, 0.0)
    before = jnp.zeros((heads, 1), F32)
    sums, ends, totals = [], [], []
    for c in range(chunks):
        rows = pl.ds(c * chunk, chunk)
        seg = precise_dot(log_ref[:, rows], upper, (1, 0))
        end = seg[:, chunk - 1 : chunk]
        flat_ref[0, :, rows] = seg
        flat_ref[1, :, rows] = jnp.exp(seg)
        flat_ref[2, :, rows] = jnp.exp(end - seg)
        flat_ref[3, :, rows] = jnp.exp(seg + before)
        sums.append(seg + before)
        before = before + end
    for c in range(chunks):
        flat_ref[4, :, pl.ds(c * chunk, chunk)] = jnp.exp(before - sums[c])
    factor = jnp.exp2(exponent_ref[...].astype(F32))
    for pair in range(pairs):
        seg_ref[pair] = jnp.zeros((COLUMN_COUNT, length), F32)
        seg_ref[pair, FACTOR : FACTOR + 1, :] = factor[pair : pair + 1, :]
        for kind in range(5):
            at = SEG + 2 * kind
            seg_ref[pair, at : at + 2, :] = flat_ref[kind, 2 * pair : 2 * pair + 2, :]

    def turn_columns(pair, _):
        col_ref[pair] = seg_ref[pair].T
        piece_decay[place, :, lanes_of(pair)] = spread_pair(
            col_ref[pair, length - 1 : length, :], FROM_START, 1
        )
        return 0

    lax.fori_loop(0, pairs, turn_columns, 0)
    for copy in decay_copies:
        copy.start()
    write_t_ref[...] = write_ref[...].astype(F32).T.astype(BF16)
    read_t_ref[...] = read_ref[...].astype(F32).T.astype(BF16)
    for c in range(chunks):
        rows = pl.ds(c * chunk, chunk)
        cross_ref[c] = dot(read_ref[rows, :], write_ref[rows, :], (1, 1))

    def unpack(pair, _):
        lanes = lanes_of(pair)
        words = packed_ref[:, lanes]
        groups = words.shape[0]
        wide = jnp.broadcast_to(words[:, None, :], (groups, 8, LANES))
        shifts = 4 * lax.broadcasted_iota(jnp.int32, (groups, 8, LANES), 1)
        fields = jnp.bitwise_and(jnp.right_shift(wide, shifts), 15) - 8
        columns = col_ref[pair]
        x = fields.astype(F32).reshape(length, LANES) * columns[:, FACTOR : FACTOR + 1]
        x_ref[:, lanes] = x.astype(BF16)
        weighted = (x * spread_pair(columns, TO_END, length)).astype(BF16)
        piece[place, :, lanes] = dot(write_t_ref[...], weighted, (1, 0)).astype(BF16)
        return 0

    bounds = [pairs * at // PARTS for at in range(PARTS + 1)]

    def piece_copy(at, step):
        span = pl.ds(bounds[at] * LANES, (bounds[at + 1] - bounds[at]) * LANES)
        return remote(
            piece.at[place, :, span], piece.at[place, :, span],
            (piece_sems.at[0, at, step - 1], piece_sems.at[1, at, step - 1]), "seq", neighbour(step),
        )

    for at in range(PARTS):
        lax.fori_loop(bounds[at], bounds[at + 1], unpack, 0)
        for step in range(1, row):
            piece_copy(at, step).start()

    def hop(at):
        span = pl.ds(bounds[at] * LANES, (bounds[at + 1] - bounds[at]) * LANES)
        return remote(
            chain_out.at[:, span], chain_in.at[:, span],
            (chain_sems.at[0, at], chain_sems.at[1, at]), "seq", me + row,
        )

    def link(at, entering):
        if at == 0:
            for copy in decay_copies:
                copy.wait_recv()
        for step in range(1, row):
            piece_copy(at, step).wait_recv()
        if entering:
            hop(at).wait_recv()

        def one(pair, _):
            lanes = lanes_of(pair)
            group, before = None, jnp.zeros((states, LANES), F32)
            scale, factor = None, jnp.ones((1, LANES), F32)
            for index in range(row):
                term = piece[index, :, lanes].astype(F32)
                decay = piece_decay[index, :, lanes]
                take = index < place
                before = jnp.where(take, term + decay * before, before)
                factor = jnp.where(take, decay * factor, factor)
                group = term if group is None else term + decay * group
                scale = decay if scale is None else decay * scale
            if entering:
                incoming = chain_in[:, lanes].astype(F32)
                group = group + scale * incoming
                before = before + factor * incoming
            state_ref[:, lanes] = before
            chain_out[:, lanes] = group.astype(BF16)
            return 0

        lax.fori_loop(bounds[at], bounds[at + 1], one, 0)

    def visit_chain(site):
        for level in range(min(4, depth)):
            here = [at for at in range(PARTS) if SITES[level][at] == site]
            is_level = z == level if level < 3 else z >= level
            if here:

                @pl.when(is_level)
                def _():
                    for at in here:
                        link(at, level > 0)

                        @pl.when(z < depth - 1)
                        def _():
                            hop(at).start()

    lane = lax.broadcasted_iota(jnp.int32, (chunk, LANES), 1)

    def local(pair, _):
        lanes = lanes_of(pair)
        state = None
        for c in range(chunks):
            part = pl.ds(c * chunk, chunk)
            columns = col_ref[pair, part, :]
            seg_rows = seg_ref[pair, :, part]
            x = x_ref[part, lanes]
            cross = cross_ref[c]
            halves = []
            for head in range(2):
                mixing = (chunk_decay(columns, seg_rows, head, chunk) * cross).astype(BF16)
                halves.append(dot(mixing, x, (1, 0)))
            y = jnp.where(lane < LANES // 2, halves[0], halves[1])
            if state is not None:
                y = y + spread_pair(columns, SEG_EXP, chunk) * dot(
                    read_ref[part, :], state.astype(BF16), (1, 0)
                )
            y_ref[part, lanes] = y
            if c < chunks - 1:
                weighted = (x.astype(F32) * spread_pair(columns, TO_CHUNK_END, chunk)).astype(BF16)
                added = dot(write_t_ref[:, part], weighted, (1, 0))
                state = (
                    added if state is None else state * chunk_scale(pair, c) + added
                )
        return 0

    third, most = pairs // 3, 3 * pairs // 4
    lax.fori_loop(0, third, local, 0)
    visit_chain(0)
    lax.fori_loop(third, most, local, 0)
    visit_chain(1)
    lax.fori_loop(most, pairs, local, 0)
    visit_chain(2)

    forwards = []
    for index, copy in enumerate(far):
        copy.wait_recv()
        source = lax.rem(mine + tensor - 2 * (index + 1), tensor)
        forwards.append(
            remote(
                part_of(source), part_of(source), (near_sems.at[0, index], near_sems.at[1, index]),
                "tp", partner,
            )
        )
        forwards[-1].start()
    near.wait_recv()
    for fetch in fetches:
        fetch.wait()
    for copy in forwards:
        copy.wait_recv()

    def pull_back(first, last):
        rows = pl.ds(first * LANES, (last - first) * LANES)
        block = dot(weight_ref[rows, :], cot_ref[...], (1, 0))
        for pair in range(first, last):
            at = (pair - first) * LANES
            grad_v_ref[:, pair * LANES : (pair + 1) * LANES] = block[at : at + LANES, :].T

    pull_back(0, pairs // 2)
    visit_chain(3)
    pull_back(pairs // 2, pairs)
    visit_chain(4)

    square_ref[...] = jnp.zeros_like(square_ref)
    inner_ref[...] = jnp.zeros_like(inner_ref)

    def mix(pair, _):
        lanes = lanes_of(pair)
        carried = dot(read_ref[...], state_ref[:, lanes].astype(BF16), (1, 0))
        y = (
            y_ref[:, lanes]
            + spread_pair(col_ref[pair], FROM_START, length) * carried
            + skip_row(pair) * x_ref[:, lanes].astype(F32)
        )
        y_ref[:, lanes] = y
        gate = gate_ref[:, lanes].astype(F32)
        mixed = y * gate * jax.nn.sigmoid(gate)
        square_ref[...] += mixed * mixed
        inner_ref[...] += grad_v_ref[:, lanes] * gain_ref[:, lanes] * mixed
        return 0

    lax.fori_loop(0, pairs, mix, 0)
    token_ref[0, 0:1, :] = jnp.sum(square_ref[...].T, axis=0, keepdims=True)
    token_ref[0, 1:2, :] = jnp.sum(inner_ref[...].T, axis=0, keepdims=True)
    token_copies = [
        remote(
            token_ref.at[0], token_ref.at[step],
            (token_sems.at[0, step - 1], token_sems.at[1, step - 1]), "tp",
            lax.rem(mine + step, tensor),
        )
        for step in range(1, tensor)
    ]
    for copy in token_copies:
        copy.start()
    for copy in token_copies:
        copy.wait_recv()
    token = token_ref[0]
    for step in range(1, tensor):
        token = token + token_ref[step]
    scale = lax.rsqrt(token[0:1, :] / (width * tensor) + 1e-05)
    pull = scale * scale * scale * token[1:2, :] / (width * tensor)
    scale_ref[...] = jnp.broadcast_to(scale, (LANES, length)).T
    pull_ref[...] = jnp.broadcast_to(pull, (LANES, length)).T

    def shape_gate(pair, _):
        lanes = lanes_of(pair)
        gain = gain_ref[:, lanes]
        y = y_ref[:, lanes]
        gate = gate_ref[:, lanes].astype(F32)
        sigma = jax.nn.sigmoid(gate)
        active = gate * sigma
        mixed = y * active
        mixed_scaled = mixed * scale_ref[...]
        normed_ref[:, lanes] = (mixed_scaled * gain).astype(BF16)
        grad_v = grad_v_ref[:, lanes]
        grad_mixed = scale_ref[...] * grad_v * gain - mixed * pull_ref[...]
        grad_gate_ref[:, lanes] = (
            grad_mixed * y * sigma * (1.0 + gate * (1.0 - sigma))
        ).astype(BF16)
        grad_y = grad_mixed * active
        grad_y_ref[:, lanes] = grad_y.astype(BF16)
        sums_ref[0:1, lanes] = jnp.sum(grad_v * mixed_scaled, axis=0, keepdims=True)
        sums_ref[1:2, lanes] = jnp.sum(grad_y * x_ref[:, lanes].astype(F32), axis=0, keepdims=True)
        weighted = (grad_y * spread_pair(col_ref[pair], FROM_START, length)).astype(BF16)
        back_piece[place, :, lanes] = dot(read_t_ref[...], weighted, (1, 0)).astype(BF16)
        return 0

    lax.fori_loop(0, pairs, shape_gate, 0)
    gate_store = pltpu.make_async_copy(grad_gate_ref, grad_gate_hbm, store_sems.at[0])
    gate_store.start()

    exchanges = [
        remote(
            back_piece.at[place], back_piece.at[place],
            (back_sems.at[0, step - 1], back_sems.at[1, step - 1]), "seq", neighbour(step),
        )
        for step in range(1, row)
    ]
    sum_copies = [
        remote(
            sums_ref, gathered.at[me], (sum_sems.at[0, step - 1], sum_sems.at[1, step - 1]), "seq",
            lax.rem(me + step, sequence),
        )
        for step in range(1, sequence)
    ]
    for copy in exchanges + sum_copies:
        copy.start()
    gathered[me] = sums_ref[...]

    def part_copy(target_z, step):
        return remote(
            part.at[target_z, step - 1], arrived.at[target_z, step - 1],
            (part_sems.at[0, target_z, step - 1], part_sems.at[1, target_z, step - 1]), "seq",
            neighbour(step),
        )

    def multiply(step, _):
        target_z = visit(z, depth, step)
        for offset in list(range(1, row)) + [0]:
            block = target_z * row + lax.rem(place + offset, row)
            taken = cot_ref[pl.ds(pl.multiple_of(block * columns_out, 16), columns_out), :]
            for at in range(0, width, 2 * LANES):
                span = pl.ds(at, min(2 * LANES, width - at))
                product = dot(taken, normed_ref[:, span], (1, 0)).astype(BF16)
                if offset:
                    part[target_z, offset - 1, :, span] = product
                else:
                    own[target_z, :, span] = product
            if offset:
                part_copy(target_z, offset).start()
        return 0

    lax.fori_loop(0, depth, multiply, 0)

    for copy in exchanges:
        copy.wait_recv()
    back_bounds = [0, (pairs + 1) // 2, pairs]
    for half in range(2):
        first, last = back_bounds[half], back_bounds[half + 1]
        span = pl.ds(first * LANES, (last - first) * LANES)
        back_hop = remote(
            back_out.at[:, span], back_in.at[:, span],
            (link_sems.at[0, half], link_sems.at[1, half]), "seq", me - row,
        )

        def back_link(entering):
            def one(pair, _):
                lanes = lanes_of(pair)
                group, after = None, jnp.zeros((back_piece.shape[1], LANES), F32)
                scale, factor = None, jnp.ones((1, LANES), F32)
                for at in reversed(range(row)):
                    term = back_piece[at, :, lanes].astype(F32)
                    decay = piece_decay[at, :, lanes]
                    take = at > place
                    after = jnp.where(take, term + decay * after, after)
                    factor = jnp.where(take, decay * factor, factor)
                    group = term if group is None else term + decay * group
                    scale = decay if scale is None else decay * scale
                if entering:
                    incoming = back_in[:, lanes].astype(F32)
                    group = group + scale * incoming
                    after = after + factor * incoming
                carry_ref[:, lanes] = after
                back_out[:, lanes] = group.astype(BF16)
                return 0

            lax.fori_loop(first, last, one, 0)

        @pl.when(z == depth - 1)
        def _():
            back_link(False)

        @pl.when(z < depth - 1)
        def _():
            back_hop.wait_recv()
            back_link(True)

        @pl.when(z > 0)
        def _():
            back_hop.start()

    def relay(step, up):
        target_z = z + (depth - 1 - step) if up else z - (depth - 1) + step
        outgoing, incoming, sems = (up_out, up_in, up_sems) if up else (down_out, down_in, down_sems)
        is_end = z == 0 if up else z == depth - 1
        is_active = z <= step if up else z >= depth - 1 - step

        def copy(at):
            return remote(
                outgoing.at[at], incoming.at[at], (sems.at[0, at], sems.at[1, at]), "seq",
                me + row if up else me - row,
            )

        def add(more):
            def one(pair, _):
                lanes = lanes_of(pair)
                value = own[target_z, :, lanes].astype(F32)
                for at in range(row - 1):
                    value = value + arrived[target_z, at, :, lanes].astype(F32)
                if more:
                    value = value + incoming[step - 1, :, lanes].astype(F32)
                outgoing[step, :, lanes] = value.astype(BF16)
                return 0

            lax.fori_loop(0, pairs, one, 0)

        @pl.when(is_end)
        def _():
            add(False)

        if step > 0:

            @pl.when(jnp.logical_and(is_active, jnp.logical_not(is_end)))
            def _():
                copy(step - 1).wait_recv()
                add(True)

        @pl.when(is_active)
        def _():
            copy(step).start()

        return copy, is_active

    def serve(step):
        target_z = visit(z, depth, step)
        for offset in range(1, row):
            part_copy(target_z, offset).wait_recv()
        return [(step,) + relay(step, True), (step,) + relay(step, False)]

    is_first = lane < LANES // 2
    half_of = lax.broadcasted_iota(jnp.int32, (8, LANES), 1)
    which = lax.broadcasted_iota(jnp.int32, (8, LANES), 0)
    select = jnp.where(lax.div(half_of, LANES // 2) == which, 1.0, 0.0)
    grad_store = pltpu.make_async_copy(grad_x_ref, grad_x_hbm, store_sems.at[1])

    def back(pair, _):
        lanes = lanes_of(pair)
        states = [state_ref[:, lanes]]
        weighted_x = []
        for c in range(chunks):
            rows = pl.ds(c * chunk, chunk)
            to_end = spread_pair(col_ref[pair, rows, :], TO_CHUNK_END, chunk)
            weighted_x.append((x_ref[rows, lanes].astype(F32) * to_end).astype(BF16))
            if c < chunks - 1:
                states.append(
                    states[-1] * chunk_scale(pair, c)
                    + dot(write_t_ref[:, rows], weighted_x[-1], (1, 0))
                )
        skip = skip_row(pair)
        carry = carry_ref[:, lanes]
        for c in reversed(range(chunks)):
            rows = pl.ds(c * chunk, chunk)
            columns = col_ref[pair, rows, :]
            seg_rows = seg_ref[pair, :, rows]
            x16 = x_ref[rows, lanes]
            x = x16.astype(F32)
            g16 = grad_y_ref[rows, lanes]
            g = g16.astype(F32)
            cross = cross_ref[c]
            state = states[c]
            chunk_exp = chunk_scale(pair, c)
            carry16 = carry.astype(BF16)
            leaving = spread_pair(columns, TO_CHUNK_END, chunk) * dot(
                write_ref[rows, :], carry16, (1, 0)
            )
            halves = []
            summed = None
            for head in range(2):
                decay = chunk_decay(columns, seg_rows, head, chunk)
                mixing = (decay * cross).astype(BF16)
                halves.append(dot(mixing, g16, (0, 0)))
                mask = is_first if head == 0 else jnp.logical_not(is_first)
                pair_dot = dot(jnp.where(mask, g, 0.0).astype(BF16), x16, (1, 1)) * decay
                summed = pair_dot if summed is None else summed + pair_dot
            summed_ref[c] += summed
            grad_x = jnp.where(is_first, halves[0], halves[1]) + leaving
            grad_x_ref[rows, lanes] = (skip * g + grad_x).astype(BF16)
            diff = g * (y_ref[rows, lanes] - skip * x) - x * grad_x
            diff_ref[rows, :] = diff
            const_ref[pair, c : c + 1, :] = jnp.sum(
                x * leaving, axis=0, keepdims=True
            ) + chunk_exp * jnp.sum(carry * state, axis=0, keepdims=True)
            weighted_g = (g * spread_pair(columns, SEG_EXP, chunk)).astype(BF16)
            map_acc[rows, :LANES] += dot(weighted_x[c], carry16, (1, 1))
            map_acc[rows, LANES:] += dot(weighted_g, state.astype(BF16), (1, 1))
            carry = carry * chunk_exp + dot(read_t_ref[:, rows], weighted_g, (1, 0))
        diff_rows[pair] = precise_dot(select, diff_ref[...], (1, 1))
        return 0

    def finish_decay(pair, _):
        const = precise_dot(select, const_ref[pair], (1, 1))
        for c in range(chunks):
            rows = pl.ds(c * chunk, chunk)
            suffix = precise_dot(diff_rows[pair, :, rows], lower, (1, 0)) + const[:, c : c + 1]
            grad_decay_ref[pair, :, rows] = suffix[0:2, :]
        return 0

    slice_rows = length // tensor

    def slice_of(index):
        return pl.ds(pl.multiple_of(index * slice_rows, 8), slice_rows)

    def scatter(step):
        peer = lax.rem(mine + step, tensor)
        return remote(
            map_acc.at[slice_of(peer)], map_in.at[step - 1],
            (map_sems.at[0, step - 1], map_sems.at[1, step - 1]), "tp", peer,
        )

    def share_copy(step):
        peer = lax.rem(mine + step, tensor)
        return remote(
            map_sum.at[slice_of(mine)], map_sum.at[slice_of(mine)],
            (share_sems.at[0, step - 1], share_sems.at[1, step - 1]), "tp", peer,
        )

    def first_half():
        map_acc[...] = jnp.zeros_like(map_acc)
        summed_ref[...] = jnp.zeros_like(summed_ref)
        const_ref[...] = jnp.zeros_like(const_ref)
        lax.fori_loop(0, (pairs + 1) // 2, back, 0)

    def second_half():
        lax.fori_loop((pairs + 1) // 2, pairs, back, 0)
        grad_store.start()
        for c in range(chunks):
            rows = pl.ds(c * chunk, chunk)
            summed = summed_ref[c].astype(BF16)
            map_acc[rows, :LANES] += dot(summed, read_ref[rows, :], (0, 0))
            map_acc[rows, LANES:] += dot(summed, write_ref[rows, :], (1, 0))
        for step in range(1, tensor):
            scatter(step).start()

    def reduce_map():
        total = map_acc[slice_of(mine), :]
        for step in range(1, tensor):
            scatter(step).wait_recv()
            total = total + map_in[step - 1]
        map_sum[slice_of(mine), :] = total
        for step in range(1, tensor):
            share_copy(step).start()
        lax.fori_loop(0, pairs, finish_decay, 0)

    work = [first_half, second_half, reduce_map]
    relays = []
    for step in range(depth - 1):
        relays += serve(step)
        if work:
            work.pop(0)()
    for task in work:
        task()

    for copy in sum_copies:
        copy.wait_recv()
    total = gathered[0]
    for at in range(1, sequence):
        total = total + gathered[at]
    total_ref[...] = total

    for offset in range(1, row):
        part_copy(z, offset).wait_recv()

    def collect(source, at, initial):
        def one(pair, _):
            lanes = lanes_of(pair)
            if initial:
                value = own[z, :, lanes].astype(F32)
                for offset in range(row - 1):
                    value = value + arrived[z, offset, :, lanes].astype(F32)
            else:
                value = acc[:, lanes] + source[at, :, lanes].astype(F32)
            acc[:, lanes] = value
            return 0

        lax.fori_loop(0, pairs, one, 0)

    collect(None, 0, True)
    last_up, last_down = relays[-2][1], relays[-1][1]

    @pl.when(z > 0)
    def _():
        last_up(depth - 2).wait_recv()
        collect(up_in, depth - 2, False)

    @pl.when(z < depth - 1)
    def _():
        last_down(depth - 2).wait_recv()
        collect(down_in, depth - 2, False)

    def turn(pair, _):
        weight_out[lanes_of(pair), :] = acc[:, lanes_of(pair)].T
        return 0

    lax.fori_loop(0, pairs, turn, 0)

    for step in range(1, tensor):
        share_copy(step).wait_recv()
    grad_write_ref[...] = map_sum[:, :LANES]
    grad_read_ref[...] = map_sum[:, LANES:]
    gate_store.wait()
    grad_store.wait()
    for step, copy, is_active in relays:

        @pl.when(is_active)
        def _():
            copy(step).wait_send()

    def sent(step, _):
        for offset in range(1, row):
            part_copy(step, offset).wait_send()
        return 0

    lax.fori_loop(0, depth, sent, 0)
    for half in range(2):
        first, last = back_bounds[half], back_bounds[half + 1]
        span = pl.ds(first * LANES, (last - first) * LANES)

        @pl.when(z > 0)
        def _():
            remote(
                back_out.at[:, span], back_in.at[:, span],
                (link_sems.at[0, half], link_sems.at[1, half]), "seq", me - row,
            ).wait_send()

    for copy in exchanges + sum_copies:
        copy.wait_send()
    for step in range(1, tensor):
        scatter(step).wait_send()
        share_copy(step).wait_send()
    for copy in far + [near] + forwards + decay_copies + token_copies:
        copy.wait_send()
    for at in range(PARTS):
        for step in range(1, row):
            piece_copy(at, step).wait_send()

        @pl.when(z < depth - 1)
        def _():
            hop(at).wait_send()


def on_device(
    packed_input,
    block_exponent,
    gate_input,
    state_write,
    state_read,
    log_decay,
    skip_weight,
    norm_gain,
    out_weight,
    out_cotangent,
):
    head_count, length = log_decay.shape
    width = packed_input.shape[1]
    states = state_write.shape[1]
    head_width = width // head_count
    pairs = width // LANES
    per_pair = head_count // pairs
    chunk = min(CHUNK, length)
    chunks = length // chunk
    sequence = lax.axis_size("seq")
    tensor = lax.axis_size("tp")
    row = chip_rows(sequence)
    depth = sequence // row
    model = out_weight.shape[1]
    share = out_cotangent.shape[1]
    cols_out = model // sequence
    block = (cols_out, width)
    hops = depth - 1
    shape = jax.ShapeDtypeStruct
    vmem = pl.BlockSpec(memory_space=pltpu.VMEM)
    smem = pl.BlockSpec(memory_space=pltpu.SMEM)
    anywhere = pl.BlockSpec(memory_space=pl.ANY)
    dma = pltpu.SemaphoreType.DMA
    buffer = pltpu.VMEM
    outs = pl.pallas_call(
        functools.partial(layer_kernel, sequence, tensor),
        in_specs=[vmem] * 3 + [smem] + [vmem] * 4 + [anywhere] * 2,
        out_specs=[anywhere] * 2 + [vmem] * 5,
        out_shape=[
            shape((length, width), BF16),
            shape((length, width), BF16),
            shape((length, states), F32),
            shape((length, states), F32),
            shape((pairs, per_pair, length), F32),
            shape((width, cols_out), F32),
            shape((2, width), F32),
        ],
        scratch_shapes=[
            buffer((length, width), BF16),
            buffer((length, width), F32),
            buffer((length, width), BF16),
            buffer((length, width), BF16),
            buffer((length, width), BF16),
            buffer((length, width), BF16),
            buffer((2, width), F32),
            buffer((states, width), F32),
            buffer((model, length), BF16),
            buffer((share, length), BF16),
            buffer((pairs, length, COLUMN_COUNT), F32),
            buffer((pairs, COLUMN_COUNT, length), F32),
            buffer((5, head_count, length), F32),
            buffer((chunks, chunk, chunk), F32),
            buffer((states, length), BF16),
            buffer((states, length), BF16),
            buffer((length, width), F32),
            buffer((length, width), BF16),
            buffer((width, model), BF16),
            buffer((row, states, width), BF16),
            buffer((row, 1, width), F32),
            buffer((states, width), BF16),
            buffer((states, width), BF16),
            buffer((length, LANES), F32),
            buffer((length, LANES), F32),
            buffer((tensor, 2, length), F32),
            buffer((length, LANES), F32),
            buffer((length, LANES), F32),
            dma((2, PARTS, row - 1)),
            dma((2, row - 1)),
            dma((2, PARTS)),
            dma((2,)),
            dma((2, tensor // 2 - 1)),
            dma((2, tensor // 2 - 1)),
            dma((2, tensor - 1)),
            dma((2,)),
            buffer((depth,) + block, BF16),
            buffer((depth, row - 1) + block, BF16),
            buffer((depth, row - 1) + block, BF16),
            buffer((hops,) + block, BF16),
            buffer((hops,) + block, BF16),
            buffer((hops,) + block, BF16),
            buffer((hops,) + block, BF16),
            buffer(block, F32),
            buffer((row, states, width), BF16),
            buffer((states, width), BF16),
            buffer((states, width), BF16),
            buffer((states, width), F32),
            buffer((sequence, 2, width), F32),
            buffer((length, 2 * states), F32),
            buffer((tensor - 1, length // tensor, 2 * states), F32),
            buffer((length, 2 * states), F32),
            buffer((chunks, chunk, chunk), F32),
            buffer((length, LANES), F32),
            buffer((pairs, 8, length), F32),
            buffer((pairs, 8, LANES), F32),
            dma((2, depth, row - 1)),
            dma((2, hops)),
            dma((2, hops)),
            dma((2, row - 1)),
            dma((2, 2)),
            dma((2, sequence - 1)),
            dma((2, tensor - 1)),
            dma((2, tensor - 1)),
            dma((2,)),
        ],
        compiler_params=pltpu.CompilerParams(
            collective_id=1, has_side_effects=True, vmem_limit_bytes=LAYER_VMEM
        ),
        cost_estimate=pl.CostEstimate(
            flops=int(130 * 9e8), bytes_accessed=int(130 * 1e5), transcendentals=0
        ),
    )(
        packed_input, block_exponent, log_decay, skip_weight, norm_gain[None], state_write,
        state_read, out_cotangent, gate_input, out_weight,
    )
    grad_input, grad_gate, grad_write, grad_read, grad_decay, grad_out_weight, totals = outs
    return (
        grad_input,
        grad_gate,
        grad_write,
        grad_read,
        grad_decay.reshape(head_count, length),
        jnp.sum(totals[1].reshape(head_count, head_width), axis=1),
        totals[0],
        grad_out_weight,
    )


def solution(mesh):
    placed = (
        P("seq", "tp"),
        P("tp", "seq"),
        P("seq", "tp"),
        P("seq", None),
        P("seq", None),
        P("tp", "seq"),
        P("tp"),
        P("tp"),
        P("tp", None),
        P("seq", "tp"),
    )
    return jax.shard_map(
        on_device,
        mesh=mesh,
        in_specs=placed,
        out_specs=(
            P("seq", "tp"),
            P("seq", "tp"),
            P("seq", None),
            P("seq", None),
            P("tp", "seq"),
            P("tp"),
            P("tp"),
            P("tp", "seq"),
        ),
        check_vma=False,
    )
```
